32 devices in a mesh: task: 4 (over y, x), tp: 8 (over z, core).
Axes of the slice: x: 2, y: 2, z: 4, core: 2. Of those that a mesh axis runs over, the one named last changes fastest.
Arguments:
- observations: bfloat16 [128, 16, 4096], P('task', None, 'tp'), may hold values from -6 to 6
- gain: float32 [4096], P('tp'), may hold values from 0.5 to 1.5
- w_in: bfloat16 [4096, 4096], P(None, 'tp'), may hold values from -0.09375 to 0.09375
- w_mix: bfloat16 [4096, 4096], P('tp'), may hold values from -0.09375 to 0.09375
- w_out: bfloat16 [4096, 4096], P(None, 'tp'), may hold values from -0.09375 to 0.09375
- w_head: bfloat16 [4096, 75], P('tp'), may hold values from -0.09375 to 0.09375
- head_bias: float32 [75], replicated, may hold values from -4 to 4
- pop_mean: float32 [57], replicated, may hold values from -8 to 8
- pop_scale: float32 [57], replicated, may hold values from 0.5 to 4
- task_indices: int32 [128], P('task'), may hold values from 0 to 56
- actions: int32 [128, 15], P('task'), may hold values from 0 to 17
- rewards: float32 [128, 15], P('task'), may hold values from -18 to 27
- episode_ends: int32 [128, 15], P('task'), may hold values 0 or 1
- behaviour_log_prob: float32 [128, 15], P('task'), may hold values from -4.5 to -1.5
Outputs:
- grad_w_in: float32 [4096, 4096], P(None, 'tp')
- grad_w_mix: float32 [4096, 4096], P('tp')
- grad_w_out: float32 [4096, 4096], P(None, 'tp')
- grad_gain: float32 [4096], P('tp')
- grad_head: float32 [4096, 75], P('tp')
- grad_head_bias: float32 [75], replicated
- new_head: bfloat16 [4096, 75], P('tp')
- new_bias: float32 [75], replicated
- updated_return_mean: float32 [57], replicated
- updated_return_scale: float32 [57], replicated
The draws below stay inside these ranges and needn't reach their ends.
All inputs are finite; a program needn't handle non-finite values. No bound on the sum of `episode_ends` on one device may be relied on, other than what follows from the above.
Results may differ from the reference program's by a relative error of at most 0.03.
Values may be sent and summed in bfloat16 or wider, within the bound.
A program may use at most 128 MiB of HBM per device.

```python
import math
import jax
import jax.numpy as jnp
from jax import lax

D = 4096
ACTIONS = 18
TASKS = 57
HEADS = 75
B_DEV = 32
FRAMES = 16
UNROLL = 15
ENVS = 128
N_TP = 8


def draw_rewards(key, part):
    group_index = (jnp.arange(ENVS, dtype=jnp.int32) // B_DEV).astype(jnp.float32)
    last_group = max(ENVS // B_DEV - 1, 1)
    rising = 1.0 + 2.0 * group_index / last_group
    sample = jnp.clip(jax.random.normal(key, (ENVS, UNROLL), jnp.float32), -4.0, 4.0)
    return sample * rising[:, None]


def set_ends(values, key, least, top_value):
    longest = values.shape.index(max(values.shape))
    spots = []
    for shift in (0, 1):
        where = [jax.random.randint(jax.random.fold_in(key, axis), (), 0, length) for axis, length in enumerate(values.shape)]
        where[longest] = (where[longest] + shift) % values.shape[longest]
        spots.append(tuple(where))
    return values.at[spots[0]].set(least).at[spots[1]].set(top_value)


def shard_levels(own_key, shape, shards, low, top_value):
    def one(axis_at, shards_of):
        heights = jax.random.uniform(jax.random.fold_in(jax.random.fold_in(own_key, 6), axis_at), (shards_of,), jnp.float32, low / len(shards), top_value / len(shards))
        return jnp.repeat(jnp.exp(heights), shape[axis_at] // shards_of).reshape((-1,) + (1,) * (len(shape) - axis_at - 1))

    loudness = one(*shards[0])
    for cut in shards[1:]:
        loudness = loudness * one(*cut)
    return loudness


def bell_draw(rng, extent, width, most, split=(), held_as=jnp.bfloat16):
    entries = width * jax.random.normal(rng, extent, jnp.float32)
    if split:
        entries = entries * shard_levels(rng, extent, split, -0.22, 0.18)
    return jnp.clip(entries, -most, most).astype(held_as)


def setup_inputs(seed: int = 0) -> dict:
    keys = jax.random.split(jax.random.key(seed), 15)
    observations = bell_draw(keys[0], (ENVS, FRAMES, D), 1.0, 6.0, ((0, 4), (2, 8)))
    gain = jnp.clip(1.0 + 0.1 * jax.random.normal(keys[1], (D,), jnp.float32), 0.5, 1.5)
    w_in = bell_draw(keys[2], (D, D), D ** -0.5, 0.09375, ((1, 8),))
    w_mix = bell_draw(keys[3], (D, D), D ** -0.5, 0.09375, ((0, 8),))
    w_out = bell_draw(keys[4], (D, D), D ** -0.5, 0.09375, ((1, 8),))
    w_head = bell_draw(keys[5], (D, HEADS), D ** -0.5, 0.09375, ((0, 8),))
    head_bias = bell_draw(keys[6], (HEADS,), 1.0, 4.0, (), jnp.float32)
    pop_mean = bell_draw(keys[7], (TASKS,), 2.0, 8.0, (), jnp.float32)
    pop_scale = jnp.clip(jnp.exp(jax.random.uniform(keys[8], (TASKS,), jnp.float32, math.log(0.5), math.log(4.0))), 0.5, 4.0)
    task_indices = set_ends(jax.random.randint(keys[9], (ENVS,), 0, TASKS), jax.random.fold_in(keys[9], 1), 0, TASKS - 1).astype(jnp.int32)
    actions = set_ends(jax.random.randint(keys[10], (ENVS, UNROLL), 0, ACTIONS), jax.random.fold_in(keys[10], 1), 0, ACTIONS - 1).astype(jnp.int32)
    rewards = draw_rewards(jax.random.fold_in(keys[14], 71), 0)
    episode_ends = set_ends((jax.random.randint(keys[12], (ENVS, UNROLL), 0, 16) < 1).astype(jnp.int32), jax.random.fold_in(keys[12], 1), 0, 1)
    behaviour_log_prob = jnp.clip(-4.5 + 3.0 * jax.random.uniform(keys[13], (ENVS, UNROLL), jnp.float32) ** shard_levels(keys[13], (ENVS, UNROLL), ((0, 4),), -0.2, 0.2), -4.5, -1.5)
    return dict(observations=observations, gain=gain, w_in=w_in, w_mix=w_mix, w_out=w_out, w_head=w_head, head_bias=head_bias, pop_mean=pop_mean, pop_scale=pop_scale, task_indices=task_indices, actions=actions, rewards=rewards, episode_ends=episode_ends, behaviour_log_prob=behaviour_log_prob)


DISCOUNT = 0.99
BASELINE_COST = 0.5
ENTROPY_COST = 0.01
POPART_PRIOR = 64.0
NORM_EPS = 1e-06

def silu_slope(before):
    sigmoid = jax.nn.sigmoid(before)
    return sigmoid * (1.0 + before * (1.0 - sigmoid))

def discounted_sums(values, factors):

    def advance(running, column):
        latest = column[0] + column[1] * running
        return (latest, latest)
    opening = jnp.zeros((values.shape[0],), jnp.float32)
    ending, stacked = lax.scan(advance, opening, (values.T, factors.T), reverse=True)
    return stacked.T

def task_onehot(task_indices):
    return (task_indices[:, None] == jnp.arange(TASKS, dtype=jnp.int32)[None, :]).astype(jnp.float32)

def popart_partials(task_indices, rewards, discount_factors):
    returns = discounted_sums(rewards, discount_factors)
    task_table = task_onehot(task_indices)
    counts = lax.optimization_barrier(jnp.sum(task_table, axis=0)) * rewards.shape[1]
    totals = jnp.dot(task_table.T, lax.optimization_barrier(jnp.sum(returns, axis=1)), precision=lax.Precision.HIGHEST)
    squares = jnp.dot(task_table.T, lax.optimization_barrier(jnp.sum(returns * returns, axis=1)), precision=lax.Precision.HIGHEST)
    return (counts, totals, squares)

def popart_update(counts, totals, squares, pop_mean, pop_scale):
    mixing = counts / (counts + POPART_PRIOR)
    safe_counts = jnp.maximum(counts, 1.0)
    batch_mean = totals / safe_counts
    batch_square = squares / safe_counts
    updated_return_mean = (1.0 - mixing) * pop_mean + mixing * batch_mean
    mean_gap = batch_mean - pop_mean
    variance = (1.0 - mixing) * pop_scale * pop_scale + mixing * (batch_square - batch_mean * batch_mean) + mixing * (1.0 - mixing) * mean_gap * mean_gap
    return (updated_return_mean, jnp.sqrt(variance))

def rescale_head(w_head, head_bias, pop_mean, pop_scale, updated_return_mean, updated_return_scale):
    scale_ratio = pop_scale / updated_return_scale
    column_scale = jnp.concatenate([jnp.ones((ACTIONS,), jnp.float32), scale_ratio])
    new_head = (w_head.astype(jnp.float32) * column_scale[None, :]).astype(jnp.bfloat16)
    value_bias = (pop_scale * head_bias[ACTIONS:] + pop_mean - updated_return_mean) / updated_return_scale
    new_bias = jnp.concatenate([head_bias[:ACTIONS], value_bias])
    return (new_head, new_bias)

def importance_trace_loss(head_value_estimates, task_indices, actions, rewards, discount_factors, behaviour_log_prob, updated_return_mean, updated_return_scale, loss_weighting):
    task_table = task_onehot(task_indices)
    env_mean = jnp.dot(task_table, updated_return_mean, precision=lax.Precision.HIGHEST)[:, None]
    env_scale = jnp.dot(task_table, updated_return_scale, precision=lax.Precision.HIGHEST)[:, None]
    logits = head_value_estimates[:, :-1, :ACTIONS]
    norm_values = lax.optimization_barrier(jnp.sum(head_value_estimates[:, :, ACTIONS:] * task_table[:, None, :], axis=2))
    values = lax.stop_gradient(norm_values * env_scale + env_mean)
    log_total = jnp.log(lax.optimization_barrier(jnp.sum(jnp.exp(logits), axis=2)))
    chosen = actions[:, :, None] == jnp.arange(ACTIONS, dtype=jnp.int32)[None, None, :]
    log_policy = lax.optimization_barrier(jnp.sum(jnp.where(chosen, logits, 0.0), axis=2)) - log_total
    clipped = jnp.minimum(jnp.exp(lax.stop_gradient(log_policy) - behaviour_log_prob), 1.0)
    deltas = clipped * (rewards + discount_factors * values[:, 1:] - values[:, :-1])
    targets = values[:, :-1] + discounted_sums(deltas, discount_factors * clipped)
    following = jnp.concatenate([targets[:, 1:], values[:, -1:]], axis=1)
    advantage = lax.stop_gradient(clipped * ((rewards + discount_factors * following - env_mean) / env_scale - norm_values[:, :-1]))
    normed_targets = lax.stop_gradient((targets - env_mean) / env_scale)
    policy = jnp.exp(logits - log_total[:, :, None])
    entropy = -lax.optimization_barrier(jnp.sum(policy * (logits - log_total[:, :, None]), axis=2))
    per_frame = -advantage * log_policy + 0.5 * BASELINE_COST * (normed_targets - norm_values[:, :-1]) ** 2 - ENTROPY_COST * entropy
    return loss_weighting * jnp.sum(per_frame)

def reference(observations, gain, w_in, w_mix, w_out, w_head, head_bias, pop_mean, pop_scale, task_indices, actions, rewards, episode_ends, behaviour_log_prob):
    env_count, frames, full_width = observations.shape
    block_width = full_width // N_TP
    row_count = env_count * frames
    tokens = observations.reshape(row_count, full_width)
    pre_in = jnp.dot(tokens, w_in, preferred_element_type=jnp.float32)
    hidden_in = jax.nn.silu(pre_in).astype(jnp.bfloat16)

    def mix_block(running, block_index):
        hidden_block = lax.dynamic_slice_in_dim(hidden_in, block_index * block_width, block_width, 1)
        weight_block = lax.dynamic_slice_in_dim(w_mix, block_index * block_width, block_width, 0)
        block_product = lax.optimization_barrier(jnp.dot(hidden_block, weight_block, preferred_element_type=jnp.float32).astype(jnp.bfloat16))
        return (running + block_product.astype(jnp.float32), None)
    mix_sum, unused = lax.scan(mix_block, jnp.zeros((row_count, full_width), jnp.float32), jnp.arange(N_TP, dtype=jnp.int32))
    residual = tokens.astype(jnp.float32) + mix_sum
    inverse = lax.rsqrt(lax.optimization_barrier(jnp.mean(residual * residual, axis=1, keepdims=True)) + NORM_EPS)
    normed = (residual * inverse * gain[None, :]).astype(jnp.bfloat16)
    pre_out = jnp.dot(normed, w_out, preferred_element_type=jnp.float32)
    hidden_out = jax.nn.silu(pre_out).astype(jnp.bfloat16)
    discount_factors = DISCOUNT * (1.0 - episode_ends.astype(jnp.float32))
    counts, totals, squares = popart_partials(task_indices, rewards, discount_factors)
    updated_return_mean, updated_return_scale = popart_update(counts, totals, squares, pop_mean, pop_scale)
    new_head, new_bias = rescale_head(w_head, head_bias, pop_mean, pop_scale, updated_return_mean, updated_return_scale)
    head_value_estimates = jnp.dot(hidden_out, new_head, preferred_element_type=jnp.float32) + new_bias[None, :]
    head_value_estimates = head_value_estimates.reshape(env_count, frames, -1)
    loss_weighting = float(ENVS) ** (-0.5)

    def whole_loss(network_outputs):
        return importance_trace_loss(network_outputs, task_indices, actions, rewards, discount_factors, behaviour_log_prob, updated_return_mean, updated_return_scale, loss_weighting)
    loss_value, pullback = jax.vjp(whole_loss, head_value_estimates)
    d_heads, = pullback(jnp.ones((), jnp.float32))
    d_rounded = d_heads.reshape(row_count, -1).astype(jnp.bfloat16)
    grad_head = jnp.dot(hidden_out.T, d_rounded, preferred_element_type=jnp.float32)
    grad_bias = lax.optimization_barrier(jnp.sum(d_rounded.astype(jnp.float32), axis=0))
    d_hidden_out = jnp.dot(d_rounded, new_head.T, preferred_element_type=jnp.float32)
    d_pre_out = (d_hidden_out * silu_slope(pre_out)).astype(jnp.bfloat16)
    grad_out = jnp.dot(normed.T, d_pre_out, preferred_element_type=jnp.float32)

    def back_block(running, block_index):
        grad_block = lax.dynamic_slice_in_dim(d_pre_out, block_index * block_width, block_width, 1)
        weight_block = lax.dynamic_slice_in_dim(w_out, block_index * block_width, block_width, 1)
        block_product = lax.optimization_barrier(jnp.dot(grad_block, weight_block.T, preferred_element_type=jnp.float32).astype(jnp.bfloat16))
        return (running + block_product.astype(jnp.float32), None)
    d_normed, unused = lax.scan(back_block, jnp.zeros((row_count, full_width), jnp.float32), jnp.arange(N_TP, dtype=jnp.int32))
    scaled = d_normed * gain[None, :]
    inner_sum = lax.optimization_barrier(jnp.sum(scaled * residual, axis=1, keepdims=True))
    d_residual = (inverse * scaled - residual * inverse ** 3 * inner_sum / full_width).astype(jnp.bfloat16)
    grad_gain = lax.optimization_barrier(jnp.sum(d_normed * residual * inverse, axis=0))
    grad_mix = jnp.dot(hidden_in.T, d_residual, preferred_element_type=jnp.float32)
    d_hidden_in = jnp.dot(d_residual, w_mix.T, preferred_element_type=jnp.float32)
    d_pre_in = (d_hidden_in * silu_slope(pre_in)).astype(jnp.bfloat16)
    grad_in = jnp.dot(tokens.T, d_pre_in, preferred_element_type=jnp.float32)
    return (grad_in, grad_mix, grad_out, grad_gain, grad_head, grad_bias, new_head, new_bias, updated_return_mean, updated_return_scale)
```

```python
import functools

import jax
import jax.numpy as jnp
from jax import lax
from jax.experimental import pallas as pl
from jax.experimental.pallas import tpu as pltpu
from jax.sharding import PartitionSpec as P

LANES = 128

ACTIONS = 18
TASKS = 57


DISCOUNT = 0.99
BASELINE_COST = 0.5
ENTROPY_COST = 0.01
POPART_PRIOR = 64.0
NORM_EPS = 1e-06


def silu_slope(before):
    sigmoid = jax.nn.sigmoid(before)
    return sigmoid * (1.0 + before * (1.0 - sigmoid))


def discounted_sums(values, factors):
    step = 1
    while step < values.shape[1]:
        pad = ((0, 0), (0, step))
        values = values + factors * jnp.pad(values[:, step:], pad)
        factors = factors * jnp.pad(factors[:, step:], pad)
        step *= 2
    return values


def task_onehot(task_indices):
    return (task_indices[:, None] == jnp.arange(TASKS, dtype=jnp.int32)[None, :]).astype(
        jnp.float32
    )


def popart_partials(task_indices, rewards, discount_factors):
    returns = discounted_sums(rewards, discount_factors)
    task_table = task_onehot(task_indices)
    counts = jnp.sum(task_table, axis=0) * rewards.shape[1]
    totals = jnp.dot(task_table.T, jnp.sum(returns, axis=1), precision=lax.Precision.HIGHEST)
    squares = jnp.dot(
        task_table.T, jnp.sum(returns * returns, axis=1), precision=lax.Precision.HIGHEST
    )
    return (counts, totals, squares)


def popart_update(counts, totals, squares, pop_mean, pop_scale):
    mixing = counts / (counts + POPART_PRIOR)
    safe_counts = jnp.maximum(counts, 1.0)
    batch_mean = totals / safe_counts
    batch_square = squares / safe_counts
    updated_return_mean = (1.0 - mixing) * pop_mean + mixing * batch_mean
    mean_gap = batch_mean - pop_mean
    variance = (
        (1.0 - mixing) * pop_scale * pop_scale
        + mixing * (batch_square - batch_mean * batch_mean)
        + mixing * (1.0 - mixing) * mean_gap * mean_gap
    )
    return (updated_return_mean, jnp.sqrt(variance))


def rescale_head(w_head, head_bias, pop_mean, pop_scale, updated_return_mean, updated_return_scale):
    scale_ratio = pop_scale / updated_return_scale
    column_scale = jnp.concatenate([jnp.ones((ACTIONS,), jnp.float32), scale_ratio])
    new_head = (w_head.astype(jnp.float32) * column_scale[None, :]).astype(jnp.bfloat16)
    value_bias = (
        pop_scale * head_bias[ACTIONS:] + pop_mean - updated_return_mean
    ) / updated_return_scale
    new_bias = jnp.concatenate([head_bias[:ACTIONS], value_bias])
    return (new_head, new_bias)


def importance_trace_loss(
    head_value_estimates,
    task_indices,
    actions,
    rewards,
    discount_factors,
    behaviour_log_prob,
    updated_return_mean,
    updated_return_scale,
    loss_weighting,
):
    task_table = task_onehot(task_indices)
    env_mean = jnp.dot(task_table, updated_return_mean, precision=lax.Precision.HIGHEST)[:, None]
    env_scale = jnp.dot(task_table, updated_return_scale, precision=lax.Precision.HIGHEST)[:, None]
    logits = head_value_estimates[:, :-1, :ACTIONS]
    norm_values = jnp.sum(head_value_estimates[:, :, ACTIONS:] * task_table[:, None, :], axis=2)
    values = lax.stop_gradient(norm_values * env_scale + env_mean)
    log_total = jnp.log(jnp.sum(jnp.exp(logits), axis=2))
    chosen = actions[:, :, None] == jnp.arange(ACTIONS, dtype=jnp.int32)[None, None, :]
    log_policy = jnp.sum(jnp.where(chosen, logits, 0.0), axis=2) - log_total
    clipped = jnp.minimum(jnp.exp(lax.stop_gradient(log_policy) - behaviour_log_prob), 1.0)
    deltas = clipped * (rewards + discount_factors * values[:, 1:] - values[:, :-1])
    targets = values[:, :-1] + discounted_sums(deltas, discount_factors * clipped)
    following = jnp.concatenate([targets[:, 1:], values[:, -1:]], axis=1)
    advantage = lax.stop_gradient(
        clipped
        * ((rewards + discount_factors * following - env_mean) / env_scale - norm_values[:, :-1])
    )
    normed_targets = lax.stop_gradient((targets - env_mean) / env_scale)
    policy = jnp.exp(logits - log_total[:, :, None])
    entropy = -jnp.sum(policy * (logits - log_total[:, :, None]), axis=2)
    per_frame = (
        -advantage * log_policy
        + 0.5 * BASELINE_COST * (normed_targets - norm_values[:, :-1]) ** 2
        - ENTROPY_COST * entropy
    )
    return loss_weighting * jnp.sum(per_frame)


def window(ref, form, slots, slot, piece, pieces):
    if form == "lanes":
        rows, width = ref.shape[0] // pieces, ref.shape[1] // slots
        start = slot * width if slots == 1 else pl.multiple_of(slot * width, width)
        return ref.at[pl.ds(piece * rows, rows), pl.ds(start, width)]
    if form == "rows":
        height = ref.shape[0] // slots
        rows = height // pieces
        return ref.at[pl.ds(pl.multiple_of(slot * height + piece * rows, rows), rows)]
    rows = ref.shape[0] // pieces
    cut = pl.ds(piece * rows, rows)
    return ref.at[cut] if slots == 1 else ref.at[cut, slot]


def greet(own, size, everyone, task_too):
    entry = pltpu.get_barrier_semaphore()
    expected = 0
    if everyone:
        for step in range(1, size):
            pl.semaphore_signal(entry, inc=1, device_id={"tp": lax.rem(own + step, size)})
        expected = size - 1
    else:
        below, above = own >= 2, own < size - 2
        pl.semaphore_signal(entry, inc=1, device_id={"tp": own + 1 - 2 * lax.rem(own, 2)})

        @pl.when(below)
        def _():
            pl.semaphore_signal(entry, inc=1, device_id={"tp": own - 2})

        @pl.when(above)
        def _():
            pl.semaphore_signal(entry, inc=1, device_id={"tp": own + 2})

        expected = 1 + below.astype(jnp.int32) + above.astype(jnp.int32)
    if task_too:
        tasks = lax.axis_size("task")
        task = lax.axis_index("task")
        for step in range(1, tasks):
            pl.semaphore_signal(entry, inc=1, device_id={"task": lax.rem(task + step, tasks)})
        expected = expected + tasks - 1
    pl.semaphore_wait(entry, expected)


RELAY_PIECES = 2


class Rider:
    def __init__(self, array, axis, mode="same", place=None, small=False):
        self.array, self.axis, self.mode, self.place = array, axis, mode, place
        self.space = pltpu.VMEM if small else pl.ANY
        self.size = 1 if mode == "mate" else lax.axis_size(axis)
        if mode == "columns":
            block = (array.shape[0], place[1])
        elif mode == "mate":
            block = array.shape[1:]
            self.size = array.shape[0]
        else:
            block = array.shape[1:]
        self.shape = jax.ShapeDtypeStruct((self.size,) + block, array.dtype)
        rows = block[0]
        self.relay = (
            not small
            and axis == "task"
            and self.size == 4
            and mode in ("same", "columns")
            and rows % (32 * RELAY_PIECES) == 0
        )
        self.pieces = RELAY_PIECES if self.relay else 1
        dma = pltpu.SemaphoreType.DMA
        if self.relay:
            self.sems = [dma((2, self.pieces)) for _ in range(4)] + [dma((1,))]
        else:
            count = 1 if mode == "mate" else max(self.size - 1, 1)
            self.sems = [dma((count,)), dma((count,)), dma((1,))]

    def bind(self, source, landed, sems):
        self.source, self.landed, self.bound = source, landed, sems
        self.own = lax.axis_index(self.axis)
        self.near = self.own + 1 - 2 * lax.rem(self.own, 2)
        self.far = self.own + 2 - 4 * lax.rem(self.own // 2, 2)
        self.across = self.near + self.far - self.own

    def view(self, target, cut=None):
        cut = pl.ds(0, self.shape.shape[1]) if cut is None else cut
        if self.mode == "columns":
            first, width = self.place
            return self.source.at[cut, pl.ds(pl.multiple_of(first() * width, width), width)]
        return self.source.at[target if self.mode == "spread" else 0, cut]

    def direct(self):
        if self.mode == "mate":
            return [
                pltpu.make_async_remote_copy(
                    src_ref=self.source,
                    dst_ref=self.landed,
                    send_sem=self.bound[0].at[0],
                    recv_sem=self.bound[1].at[0],
                    device_id={"tp": self.near},
                )
            ]
        copies = []
        for step in range(1, self.size):
            target = lax.rem(self.own + step, self.size)
            copies.append(
                pltpu.make_async_remote_copy(
                    src_ref=self.view(target),
                    dst_ref=self.landed.at[self.own],
                    send_sem=self.bound[0].at[step - 1],
                    recv_sem=self.bound[1].at[step - 1],
                    device_id={self.axis: target},
                )
            )
        return copies

    def keep(self):
        return pltpu.make_async_copy(
            self.view(self.own), self.landed.at[self.own], self.bound[-1].at[0]
        )

    def rows(self, piece, half=None):
        length = self.shape.shape[1] // self.pieces
        if half is None:
            return pl.ds(piece * length, length)
        return pl.ds(piece * length + half * (length // 2), length // 2)

    def first_hop(self, way, piece):
        return pltpu.make_async_remote_copy(
            src_ref=self.view(0, self.rows(piece)),
            dst_ref=self.landed.at[self.own, self.rows(piece)],
            send_sem=self.bound[0].at[way, piece],
            recv_sem=self.bound[1].at[way, piece],
            device_id={"task": self.far if way else self.near},
        )

    def second_hop(self, way, piece):
        place = self.landed.at[self.far if way else self.near, self.rows(piece, way)]
        return pltpu.make_async_remote_copy(
            src_ref=place,
            dst_ref=place,
            send_sem=self.bound[2].at[way, piece],
            recv_sem=self.bound[3].at[way, piece],
            device_id={"task": self.near if way else self.far},
        )

    def start(self):
        if self.relay:
            for piece in range(self.pieces):
                for way in (0, 1):
                    self.first_hop(way, piece).start()
        else:
            for copy in self.direct():
                copy.start()
        if self.mode != "mate":
            self.keep().start()

    def advance(self, piece):
        if self.relay and piece < self.pieces:
            for way in (0, 1):
                self.first_hop(way, piece).wait_recv()
                self.second_hop(way, piece).start()

    def finish(self):
        if self.mode != "mate":
            self.keep().wait()
        if self.relay:
            for piece in range(self.pieces):
                for way in (0, 1):
                    self.first_hop(way, piece).wait_send()
                    self.second_hop(way, piece).wait()
        else:
            for copy in self.direct():
                copy.wait()


def bind_riders(riders, refs):
    count = len(riders)
    sems = list(refs[2 * count :])
    for i, rider in enumerate(riders):
        taken = len(rider.sems)
        rider.bind(refs[i], refs[count + i], sems[:taken])
        sems = sems[taken:]


def rider_greeting(riders):
    tp_wide = any(r.axis == "tp" and r.mode != "mate" for r in riders)
    return tp_wide, any(r.axis == "task" for r in riders)


def line_gather_kernel(size, form, pieces, riders, *refs):
    count = len(riders)
    source, landed = refs[0], refs[1 + count]
    sems = refs[2 + 2 * count :]
    up_send, up_recv, down_send, down_recv, mate_send, mate_recv, own_sem = sems[:7]
    bind_riders(riders, refs[1 : 1 + count] + refs[2 + count : 2 + 2 * count] + sems[7:])
    own = lax.axis_index("tp")
    core, site, sites = lax.rem(own, 2), own // 2, size // 2
    mate = own + 1 - 2 * core
    greet(own, size, *rider_greeting(riders))

    def hop(step, piece, ahead, origin):
        slot = 2 * origin + core
        place = window(landed, form, size, slot, piece, pieces)
        start = window(source, form, 1, 0, piece, pieces) if step == 0 else place
        return pltpu.make_async_remote_copy(
            src_ref=start,
            dst_ref=place,
            send_sem=(up_send if ahead else down_send).at[step, piece],
            recv_sem=(up_recv if ahead else down_recv).at[step, piece],
            device_id={"tp": own + 2 if ahead else own - 2},
        )

    def pass_on(origin, piece, first):
        place = window(landed, form, size, 2 * origin + core, piece, pieces)
        return pltpu.make_async_remote_copy(
            src_ref=window(source, form, 1, 0, piece, pieces) if first else place,
            dst_ref=place,
            send_sem=mate_send.at[origin, piece],
            recv_sem=mate_recv.at[origin, piece],
            device_id={"tp": mate},
        )

    for piece in range(pieces):

        @pl.when(site < sites - 1)
        def _():
            hop(0, piece, True, site).start()

        @pl.when(site > 0)
        def _():
            hop(0, piece, False, site).start()

    for rider in riders:
        rider.start()
    keep = []
    for piece in range(pieces):
        pass_on(site, piece, True).start()
        copy = pltpu.make_async_copy(
            window(source, form, 1, 0, piece, pieces),
            window(landed, form, size, own, piece, pieces),
            own_sem.at[piece],
        )
        copy.start()
        keep.append(copy)
    for step in range(1, sites):
        for piece in range(pieces):

            @pl.when(site >= step)
            def _():
                hop(step - 1, piece, True, site - step).wait_recv()

                @pl.when(site < sites - 1)
                def _():
                    hop(step, piece, True, site - step).start()

                pass_on(site - step, piece, False).start()

            @pl.when(site + step < sites)
            def _():
                hop(step - 1, piece, False, site + step).wait_recv()

                @pl.when(site > 0)
                def _():
                    hop(step, piece, False, site + step).start()

                pass_on(site + step, piece, False).start()

        for rider in riders:
            rider.advance(step - 1)

    for step in range(sites - 1, RELAY_PIECES + 1):
        for rider in riders:
            rider.advance(step)
    for copy in keep:
        copy.wait()
    for step in range(sites - 1):
        for piece in range(pieces):

            @pl.when((site >= step) & (site < sites - 1))
            def _():
                hop(step, piece, True, site - step).wait_send()

            @pl.when((site + step < sites) & (site > 0))
            def _():
                hop(step, piece, False, site + step).wait_send()

    for origin in range(sites):
        for piece in range(pieces):
            pass_on(origin, piece, False).wait()

    for rider in riders:
        rider.finish()


def line_gather(block, form, identity, riders=()):
    size = lax.axis_size("tp")
    shape = list(block.shape)
    if form == "cross":
        shape = shape[:1] + [size] + shape[1:]
    else:
        shape[1 if form == "lanes" else 0] *= size
    pieces = 2 if block.shape[0] % 2 == 0 else 1
    sites = size // 2
    dma = pltpu.SemaphoreType.DMA
    anywhere = pl.BlockSpec(memory_space=pl.ANY)
    specs = [anywhere] + [pl.BlockSpec(memory_space=r.space) for r in riders]
    return pl.pallas_call(
        functools.partial(line_gather_kernel, size, form, pieces, riders),
        out_shape=[jax.ShapeDtypeStruct(tuple(shape), block.dtype)] + [r.shape for r in riders],
        in_specs=specs,
        out_specs=specs,
        scratch_shapes=[dma((max(sites - 1, 1), pieces)) for _ in range(4)]
        + [dma((sites, pieces)), dma((sites, pieces)), dma((pieces,))]
        + [sem for r in riders for sem in r.sems],
        compiler_params=pltpu.CompilerParams(
            collective_id=identity, has_side_effects=True, vmem_limit_bytes=16 * 1024 * 1024
        ),
        cost_estimate=pl.CostEstimate(
            flops=10_000_000_000, bytes_accessed=2 * size * block.size, transcendentals=0
        ),
        name="line_gather",
    )(block, *[r.array for r in riders])


def line_scatter_kernel(size, pieces, riders, *refs):
    count = len(riders)
    terms, total = refs[0], refs[1 + count]
    riding = refs[1 : 1 + count] + refs[2 + count : 2 + 2 * count] + refs[2 + 2 * count + 11 :]
    bind_riders(riders, riding)
    refs = refs[2 + 2 * count : 2 + 2 * count + 11]
    mate_in, up_in, down_in, up_out, down_out = refs[:5]
    mate_send, mate_recv, up_send, up_recv, down_send, down_recv = refs[5:]
    own = lax.axis_index("tp")
    core, site, sites = lax.rem(own, 2), own // 2, size // 2
    mate = own + 1 - 2 * core
    rows = terms.shape[1] // pieces
    greet(own, size, *rider_greeting(riders))

    def cut(piece):
        return pl.ds(piece * rows, rows)

    def to_mate(site_of, piece):
        return pltpu.make_async_remote_copy(
            src_ref=terms.at[2 * site_of + 1 - core, cut(piece)],
            dst_ref=mate_in.at[site_of, cut(piece)],
            send_sem=mate_send.at[site_of, piece],
            recv_sem=mate_recv.at[site_of, piece],
            device_id={"tp": mate},
        )

    def hop(site_of, piece, ahead):
        return pltpu.make_async_remote_copy(
            src_ref=(up_out if ahead else down_out).at[site_of, cut(piece)],
            dst_ref=(up_in if ahead else down_in).at[site_of, cut(piece)],
            send_sem=(up_send if ahead else down_send).at[site_of, piece],
            recv_sem=(up_recv if ahead else down_recv).at[site_of, piece],
            device_id={"tp": own + 2 if ahead else own - 2},
        )

    def pair_sum(site_of, piece):
        return terms[2 * site_of + core, cut(piece)].astype(jnp.float32) + mate_in[
            site_of, cut(piece)
        ].astype(jnp.float32)

    order = []
    for far in range((sites + 1) // 2):
        order += [sites - 1 - far] + ([far] if far != sites - 1 - far else [])
    for site_of in order:
        for piece in range(pieces):
            to_mate(site_of, piece).start()
    for rider in riders:
        rider.start()
    for far in range(sites - 1):
        for piece in range(pieces):
            for ahead, site_of in ((True, sites - 1 - far), (False, far)):
                arriving = (site > 0) if ahead else (site < sites - 1)
                outbox = up_out if ahead else down_out
                inbox = up_in if ahead else down_in

                @pl.when((site_of > site) if ahead else (site_of < site))
                def _():
                    to_mate(site_of, piece).wait_recv()

                    @pl.when(arriving)
                    def _():
                        hop(site_of, piece, ahead).wait_recv()
                        outbox[site_of, cut(piece)] = (
                            pair_sum(site_of, piece) + inbox[site_of, cut(piece)].astype(jnp.float32)
                        ).astype(outbox.dtype)

                    @pl.when(jnp.logical_not(arriving))
                    def _():
                        outbox[site_of, cut(piece)] = pair_sum(site_of, piece).astype(outbox.dtype)

                    hop(site_of, piece, ahead).start()

        for rider in riders:
            rider.advance(far)

    for step in range(sites - 1, RELAY_PIECES + 1):
        for rider in riders:
            rider.advance(step)
    for piece in range(pieces):
        to_mate(site, piece).wait_recv()
        total[cut(piece)] = pair_sum(site, piece)

        @pl.when(site > 0)
        def _():
            hop(site, piece, True).wait_recv()
            total[cut(piece)] += up_in[site, cut(piece)].astype(jnp.float32)

        @pl.when(site < sites - 1)
        def _():
            hop(site, piece, False).wait_recv()
            total[cut(piece)] += down_in[site, cut(piece)].astype(jnp.float32)

    for site_of in range(sites):
        for piece in range(pieces):
            to_mate(site_of, piece).wait_send()

            @pl.when(site_of > site)
            def _():
                hop(site_of, piece, True).wait_send()

            @pl.when(site_of < site)
            def _():
                hop(site_of, piece, False).wait_send()

    for rider in riders:
        rider.finish()


def line_scatter(terms, identity, riders=()):
    size = lax.axis_size("tp")
    sites = size // 2
    rows, width = terms.shape[1:]
    pieces = 2 if rows % 32 == 0 else 1
    dma = pltpu.SemaphoreType.DMA
    box = pltpu.VMEM((sites, rows, width), terms.dtype)
    vmem = pl.BlockSpec(memory_space=pltpu.VMEM)
    specs = [vmem] + [pl.BlockSpec(memory_space=r.space) for r in riders]
    return pl.pallas_call(
        functools.partial(line_scatter_kernel, size, pieces, riders),
        out_shape=[jax.ShapeDtypeStruct((rows, width), jnp.float32)] + [r.shape for r in riders],
        in_specs=specs,
        out_specs=specs,
        scratch_shapes=[box] * 5
        + [dma((sites, pieces))] * 6
        + [sem for r in riders for sem in r.sems],
        compiler_params=pltpu.CompilerParams(
            collective_id=identity, has_side_effects=True, vmem_limit_bytes=32 * 1024 * 1024
        ),
        cost_estimate=pl.CostEstimate(
            flops=10_000_000_000, bytes_accessed=4 * terms.size, transcendentals=0
        ),
        name="line_scatter",
    )(terms, *[r.array for r in riders])


def exchange_kernel(axis, size, spread, source, landed, send_sems, recv_sems):
    own = lax.axis_index(axis)
    entry = pltpu.get_barrier_semaphore()
    for step in range(1, size):
        pl.semaphore_signal(entry, inc=1, device_id={axis: lax.rem(own + step, size)})
    pl.semaphore_wait(entry, size - 1)
    copies = []
    for step in range(1, size):
        target = lax.rem(own + step, size)
        copy = pltpu.make_async_remote_copy(
            src_ref=source.at[target if spread else 0],
            dst_ref=landed.at[own],
            send_sem=send_sems.at[step - 1],
            recv_sem=recv_sems.at[step - 1],
            device_id={axis: target},
        )
        copy.start()
        copies.append(copy)
    landed[own] = source[own if spread else 0]
    for copy in copies:
        copy.wait()


def exchange(blocks, axis, spread, identity):
    size = lax.axis_size(axis)
    return pl.pallas_call(
        functools.partial(exchange_kernel, axis, size, spread),
        out_shape=jax.ShapeDtypeStruct((size,) + blocks.shape[1:], blocks.dtype),
        in_specs=[pl.BlockSpec(memory_space=pltpu.VMEM)],
        out_specs=pl.BlockSpec(memory_space=pltpu.VMEM),
        scratch_shapes=[
            pltpu.SemaphoreType.DMA((size - 1,)),
            pltpu.SemaphoreType.DMA((size - 1,)),
        ],
        compiler_params=pltpu.CompilerParams(
            collective_id=identity, has_side_effects=True, vmem_limit_bytes=8 * 1024 * 1024
        ),
        cost_estimate=pl.CostEstimate(
            flops=400_000_000, bytes_accessed=2 * blocks.size, transcendentals=0
        ),
    )(blocks)


def task_gather(value):
    tasks, own = lax.axis_size("task"), lax.axis_index("task")
    found = [(own, value)]
    for step in range(1, tasks):
        if tasks & (tasks - 1):
            pairs, origin = [(i, (i + step) % tasks) for i in range(tasks)], (own - step) % tasks
        else:
            pairs, origin = [(i, i ^ step) for i in range(tasks)], own ^ step
        found.append((origin, lax.ppermute(value, "task", pairs)))
    return found


def on_device(
    observations,
    gain,
    w_in,
    w_mix,
    w_out,
    w_head,
    head_bias,
    pop_mean,
    pop_scale,
    task_indices,
    actions,
    rewards,
    episode_ends,
    behaviour_log_prob,
):
    env_count, frames, part_width = observations.shape
    groups = lax.axis_size("tp")
    full_width = part_width * groups
    row_count = env_count * frames
    local_rows = row_count // groups
    own_tokens = observations.reshape(row_count, part_width)
    discount_factors = DISCOUNT * (1.0 - episode_ends.astype(jnp.float32))
    counts, totals, squares = popart_partials(task_indices, rewards, discount_factors)
    count_tasks = counts.shape[0]
    sums = jnp.stack([counts, totals, squares])
    sums = jnp.pad(sums, ((0, 5), (0, -count_tasks % LANES)))
    own_slot = lax.axis_index("tp")
    core, sites = lax.rem(own_slot, 2), groups // 2

    def slot_away(away):
        own_now = lax.axis_index("tp")
        return 2 * lax.rem(own_now // 2 + away, sites) + lax.rem(own_now, 2)

    def token_rider(away):
        return Rider(tokens, "task", "columns", (lambda: slot_away(away), part_width))

    tokens, gain_all, token_block = line_gather(
        own_tokens,
        "lanes",
        0,
        (Rider(gain.reshape(1, -1, LANES), "tp", small=True), Rider(own_tokens[None], "task")),
    )
    token_blocks = [token_block]
    row_offset = lax.axis_index("tp") * local_rows
    token_rows = lax.dynamic_slice_in_dim(tokens, row_offset, local_rows, 0)
    pre_in = jnp.dot(tokens, w_in, preferred_element_type=jnp.float32)
    hidden_in = jax.nn.silu(pre_in).astype(jnp.bfloat16)
    mix_terms = jnp.dot(hidden_in, w_mix, preferred_element_type=jnp.float32).astype(jnp.bfloat16)
    mix_sum, all_sums, hidden_all, *blocks = line_scatter(
        mix_terms.reshape(groups, local_rows, full_width),
        1,
        (Rider(sums[None], "task", small=True), Rider(hidden_in[None], "task"))
        + tuple(token_rider(away) for away in range(1, min(sites, 2))),
    )
    token_blocks += blocks
    gain_all = gain_all.reshape(full_width)
    counts, totals, squares = jnp.sum(all_sums, axis=0)[:3, :count_tasks]
    updated_return_mean, updated_return_scale = popart_update(
        counts, totals, squares, pop_mean, pop_scale
    )
    new_head, new_bias = rescale_head(
        w_head, head_bias, pop_mean, pop_scale, updated_return_mean, updated_return_scale
    )
    loss_weighting = float(env_count * lax.axis_size("task")) ** (-0.5)
    heads = new_head.shape[1]
    wide_head = jnp.pad(new_head, ((0, 0), (0, -heads % LANES)))
    residual = token_rows.astype(jnp.float32) + mix_sum
    inverse = lax.rsqrt(jnp.mean(residual * residual, axis=1, keepdims=True) + NORM_EPS)
    normed = (residual * inverse * gain_all[None, :]).astype(jnp.bfloat16)
    normed_all, *blocks = line_gather(
        normed, "rows", 2, tuple(token_rider(away) for away in range(2, sites))
    )
    token_blocks += blocks
    pre_out = jnp.dot(normed_all, w_out, preferred_element_type=jnp.float32)
    hidden_out = jax.nn.silu(pre_out).astype(jnp.bfloat16)
    head_terms = jnp.dot(hidden_out, wide_head, preferred_element_type=jnp.float32)
    head_blocks = head_terms.astype(jnp.bfloat16).reshape(groups, local_rows, -1)
    head_sum = jnp.sum(exchange(head_blocks, "tp", True, 3).astype(jnp.float32), axis=0)
    head_value_estimates = head_sum[:, :heads] + new_bias[None, :]
    own_envs = env_count // groups
    head_value_estimates = head_value_estimates.reshape(own_envs, frames, heads)

    def own(values):
        return lax.dynamic_slice_in_dim(values, lax.axis_index("tp") * own_envs, own_envs, 0)

    def group_loss(network_outputs):
        return importance_trace_loss(
            network_outputs,
            own(task_indices),
            own(actions),
            own(rewards),
            own(discount_factors),
            own(behaviour_log_prob),
            updated_return_mean,
            updated_return_scale,
            loss_weighting,
        )

    loss_value, pullback = jax.vjp(group_loss, head_value_estimates)
    (d_heads,) = pullback(jnp.ones((), jnp.float32))
    d_own = d_heads.reshape(local_rows, heads).astype(jnp.bfloat16)
    d_own = jnp.pad(d_own, ((0, 0), (0, -heads % LANES)))
    d_rounded = exchange(d_own[None], "tp", False, 4).reshape(row_count, -1)
    d_hidden_out = jnp.dot(d_rounded, wide_head.T, preferred_element_type=jnp.float32)
    d_pre_out = (d_hidden_out * silu_slope(pre_out)).astype(jnp.bfloat16)
    d_terms = jnp.dot(d_pre_out, w_out.T, preferred_element_type=jnp.float32)
    d_terms = d_terms.astype(jnp.bfloat16)
    grad_out = jnp.dot(normed_all.T, d_pre_out, preferred_element_type=jnp.float32)
    grad_head = jnp.dot(hidden_out.T, d_rounded, preferred_element_type=jnp.float32)
    grad_bias = jnp.sum(d_rounded.astype(jnp.float32), axis=0)
    tasks = lax.axis_size("task")
    out_quarter, quarter = full_width // tasks, full_width // tasks
    d_normed, grad_out, grad_head = line_scatter(
        d_terms.reshape(groups, local_rows, full_width),
        5,
        (
            Rider(
                grad_out.astype(jnp.bfloat16).reshape(tasks, out_quarter, part_width),
                "task",
                "spread",
            ),
            Rider(grad_head.astype(jnp.bfloat16)[None], "task", small=True),
        ),
    )
    grad_out = jnp.sum(grad_out.astype(jnp.float32), axis=0).astype(jnp.bfloat16)
    grad_head = jnp.sum(grad_head.astype(jnp.float32), axis=0)[:, :heads]
    scaled = d_normed * gain_all[None, :]
    inner_sum = jnp.sum(scaled * residual, axis=1, keepdims=True)
    d_residual = (inverse * scaled - residual * inverse**3 * inner_sum / full_width).astype(
        jnp.bfloat16
    )
    gain_terms = jnp.sum(d_normed * residual * inverse, axis=0).reshape(groups, -1, LANES)
    d_quarters = d_residual.reshape(local_rows, tasks, quarter).transpose(1, 0, 2)
    arrived, gain_blocks, grad_out, d_quarters = line_gather(
        d_residual,
        "rows",
        6,
        (
            Rider(gain_terms, "tp", "spread", small=True),
            Rider(grad_out[None], "task"),
            Rider(d_quarters, "task", "spread"),
        ),
    )
    d_hidden = jnp.dot(arrived, w_mix.T, preferred_element_type=jnp.float32)
    d_pre_in = (d_hidden * silu_slope(pre_in)).astype(jnp.bfloat16)
    gain_block = jnp.sum(gain_blocks, axis=0)
    bias_block = grad_bias.reshape(-1, LANES)
    small = jnp.concatenate([gain_block, bias_block], axis=0)
    small = jnp.pad(small, ((0, -small.shape[0] % 8), (0, 0)))
    d_cross, d_pre_in, small, *mate_blocks = line_gather(
        d_quarters,
        "cross",
        7,
        (Rider(d_pre_in[None], "task"), Rider(small[None], "task", small=True))
        + tuple(Rider(block, "tp", "mate") for block in token_blocks),
    )
    small = jnp.sum(small, axis=0)
    gain_rows = gain_block.shape[0]
    grad_gain = small[:gain_rows].reshape(part_width)
    grad_bias = small[gain_rows : gain_rows + bias_block.shape[0]].reshape(-1)[:heads]
    every_row = tasks * row_count
    grad_mix = jnp.dot(
        hidden_all.reshape(every_row, part_width).T,
        d_cross.reshape(every_row, quarter),
        preferred_element_type=jnp.float32,
    )
    grad_mix, d_pre_in, grad_out = lax.optimization_barrier(
        (grad_mix.astype(jnp.bfloat16), d_pre_in, grad_out)
    )
    mix_found = task_gather(grad_mix)
    grad_in = jnp.zeros((full_width, part_width), jnp.float32)
    d_pre_in = d_pre_in.reshape(every_row, part_width)
    for away in range(sites):
        for block, slot in (
            (token_blocks[away], slot_away(away)),
            (mate_blocks[away], slot_away(away) + 1 - 2 * core),
        ):
            rows = jnp.dot(
                block.reshape(every_row, part_width).T,
                d_pre_in,
                preferred_element_type=jnp.float32,
            )
            grad_in = lax.dynamic_update_slice_in_dim(grad_in, rows, slot * part_width, 0)
    grad_out = grad_out.reshape(full_width, part_width).astype(jnp.float32)
    arrivals, grad_in, grad_out = lax.optimization_barrier(
        ([value for _, value in mix_found], grad_in, grad_out)
    )
    grad_mix = jnp.zeros((part_width, full_width), jnp.float32)
    for (task, _), value in zip(mix_found, arrivals):
        grad_mix = lax.dynamic_update_slice_in_dim(
            grad_mix, value.astype(jnp.float32), task * quarter, 1
        )
    return (
        grad_in,
        grad_mix,
        grad_out,
        grad_gain,
        grad_head,
        grad_bias,
        new_head,
        new_bias,
        updated_return_mean,
        updated_return_scale,
    )


def solution(mesh):
    in_specs = (
        P("task", None, "tp"),
        P("tp"),
        P(None, "tp"),
        P("tp", None),
        P(None, "tp"),
        P("tp", None),
        P(),
        P(),
        P(),
        P("task"),
        P("task", None),
        P("task", None),
        P("task", None),
        P("task", None),
    )
    out_specs = (
        P(None, "tp"),
        P("tp", None),
        P(None, "tp"),
        P("tp"),
        P("tp", None),
        P(),
        P("tp", None),
        P(),
        P(),
        P(),
    )
    return jax.shard_map(
        on_device, mesh=mesh, in_specs=in_specs, out_specs=out_specs, check_vma=False
    )
```

```python
import functools

import jax
import jax.numpy as jnp
from jax import lax
from jax.experimental import pallas as pl
from jax.experimental.pallas import tpu as pltpu
from jax.sharding import PartitionSpec as P

LANES = 128

ACTIONS = 18
TASKS = 57


DISCOUNT = 0.99
BASELINE_COST = 0.5
ENTROPY_COST = 0.01
POPART_PRIOR = 64.0
NORM_EPS = 1e-06


def silu_slope(before):
    sigmoid = jax.nn.sigmoid(before)
    return sigmoid * (1.0 + before * (1.0 - sigmoid))


def discounted_sums(values, factors):
    step = 1
    while step < values.shape[1]:
        pad = ((0, 0), (0, step))
        values = values + factors * jnp.pad(values[:, step:], pad)
        factors = factors * jnp.pad(factors[:, step:], pad)
        step *= 2
    return values


def task_onehot(task_indices):
    return (task_indices[:, None] == jnp.arange(TASKS, dtype=jnp.int32)[None, :]).astype(
        jnp.float32
    )


def popart_partials(task_indices, rewards, discount_factors):
    returns = discounted_sums(rewards, discount_factors)
    task_table = task_onehot(task_indices)
    counts = jnp.sum(task_table, axis=0) * rewards.shape[1]
    totals = jnp.dot(task_table.T, jnp.sum(returns, axis=1), precision=lax.Precision.HIGHEST)
    squares = jnp.dot(
        task_table.T, jnp.sum(returns * returns, axis=1), precision=lax.Precision.HIGHEST
    )
    return (counts, totals, squares)


def popart_update(counts, totals, squares, pop_mean, pop_scale):
    mixing = counts / (counts + POPART_PRIOR)
    safe_counts = jnp.maximum(counts, 1.0)
    batch_mean = totals / safe_counts
    batch_square = squares / safe_counts
    updated_return_mean = (1.0 - mixing) * pop_mean + mixing * batch_mean
    mean_gap = batch_mean - pop_mean
    variance = (
        (1.0 - mixing) * pop_scale * pop_scale
        + mixing * (batch_square - batch_mean * batch_mean)
        + mixing * (1.0 - mixing) * mean_gap * mean_gap
    )
    return (updated_return_mean, jnp.sqrt(variance))


def rescale_head(w_head, head_bias, pop_mean, pop_scale, updated_return_mean, updated_return_scale):
    scale_ratio = pop_scale / updated_return_scale
    column_scale = jnp.concatenate([jnp.ones((ACTIONS,), jnp.float32), scale_ratio])
    new_head = (w_head.astype(jnp.float32) * column_scale[None, :]).astype(jnp.bfloat16)
    value_bias = (
        pop_scale * head_bias[ACTIONS:] + pop_mean - updated_return_mean
    ) / updated_return_scale
    new_bias = jnp.concatenate([head_bias[:ACTIONS], value_bias])
    return (new_head, new_bias)


def importance_trace_loss(
    head_value_estimates,
    task_indices,
    actions,
    rewards,
    discount_factors,
    behaviour_log_prob,
    updated_return_mean,
    updated_return_scale,
    loss_weighting,
):
    task_table = task_onehot(task_indices)
    env_mean = jnp.dot(task_table, updated_return_mean, precision=lax.Precision.HIGHEST)[:, None]
    env_scale = jnp.dot(task_table, updated_return_scale, precision=lax.Precision.HIGHEST)[:, None]
    logits = head_value_estimates[:, :-1, :ACTIONS]
    norm_values = jnp.sum(head_value_estimates[:, :, ACTIONS:] * task_table[:, None, :], axis=2)
    values = lax.stop_gradient(norm_values * env_scale + env_mean)
    log_total = jnp.log(jnp.sum(jnp.exp(logits), axis=2))
    chosen = actions[:, :, None] == jnp.arange(ACTIONS, dtype=jnp.int32)[None, None, :]
    log_policy = jnp.sum(jnp.where(chosen, logits, 0.0), axis=2) - log_total
    clipped = jnp.minimum(jnp.exp(lax.stop_gradient(log_policy) - behaviour_log_prob), 1.0)
    deltas = clipped * (rewards + discount_factors * values[:, 1:] - values[:, :-1])
    targets = values[:, :-1] + discounted_sums(deltas, discount_factors * clipped)
    following = jnp.concatenate([targets[:, 1:], values[:, -1:]], axis=1)
    advantage = lax.stop_gradient(
        clipped
        * ((rewards + discount_factors * following - env_mean) / env_scale - norm_values[:, :-1])
    )
    normed_targets = lax.stop_gradient((targets - env_mean) / env_scale)
    policy = jnp.exp(logits - log_total[:, :, None])
    entropy = -jnp.sum(policy * (logits - log_total[:, :, None]), axis=2)
    per_frame = (
        -advantage * log_policy
        + 0.5 * BASELINE_COST * (normed_targets - norm_values[:, :-1]) ** 2
        - ENTROPY_COST * entropy
    )
    return loss_weighting * jnp.sum(per_frame)


def window(ref, form, slots, slot, piece, pieces):
    if form == "lanes":
        rows, width = ref.shape[0] // pieces, ref.shape[1] // slots
        start = slot * width if slots == 1 else pl.multiple_of(slot * width, width)
        return ref.at[pl.ds(piece * rows, rows), pl.ds(start, width)]
    if form == "rows":
        height = ref.shape[0] // slots
        rows = height // pieces
        return ref.at[pl.ds(pl.multiple_of(slot * height + piece * rows, rows), rows)]
    rows = ref.shape[-2] // pieces
    cut = pl.ds(piece * rows, rows)
    return ref.at[:, cut] if slots == 1 else ref.at[:, slot, cut]


def greet(own, size, everyone, task_too):
    entry = pltpu.get_barrier_semaphore()
    expected = 0
    if everyone:
        for step in range(1, size):
            pl.semaphore_signal(entry, inc=1, device_id={"tp": lax.rem(own + step, size)})
        expected = size - 1
    else:
        below, above = own >= 2, own < size - 2
        pl.semaphore_signal(entry, inc=1, device_id={"tp": own + 1 - 2 * lax.rem(own, 2)})

        @pl.when(below)
        def _():
            pl.semaphore_signal(entry, inc=1, device_id={"tp": own - 2})

        @pl.when(above)
        def _():
            pl.semaphore_signal(entry, inc=1, device_id={"tp": own + 2})

        expected = 1 + below.astype(jnp.int32) + above.astype(jnp.int32)
    if task_too:
        tasks = lax.axis_size("task")
        task = lax.axis_index("task")
        for step in range(1, tasks):
            pl.semaphore_signal(entry, inc=1, device_id={"task": lax.rem(task + step, tasks)})
        expected = expected + tasks - 1
    pl.semaphore_wait(entry, expected)


RELAY_PIECES = 2


class Rider:
    def __init__(self, array, axis, mode="same", slots=None, width=None, carry=None, small=False):
        self.axis, self.mode, self.small = axis, mode, small
        self.size = lax.axis_size(axis)
        self.carry = carry
        self.inputs = [] if array is None else [array]
        self.inputs += [] if carry is None else [carry]
        self.slots = slots
        self.width = width
        dma = pltpu.SemaphoreType.DMA
        if mode == "mate":
            self.shape = jax.ShapeDtypeStruct(carry.shape, carry.dtype)
            self.relay, self.pieces, self.count = False, 0, self.size // 2
            self.scratch = [dma((self.count,)), dma((self.count,))]
            return
        block = (array.shape[0], width) if mode == "columns" else array.shape[1:]
        self.block = block
        shape = (self.size,) + block
        if slots is not None:
            self.width = block[-1]
            shape = shape[:-1] + (lax.axis_size("tp") * self.width,)
        self.shape = jax.ShapeDtypeStruct(shape, array.dtype)
        self.relay = (
            not small
            and axis == "task"
            and self.size == 4
            and mode in ("same", "columns")
            and block[0] % (32 * RELAY_PIECES) == 0
        )
        self.count = 1 if slots is None else len(slots)
        self.pieces = RELAY_PIECES * self.count if self.relay else 0
        if self.relay:
            self.scratch = [dma((2, self.pieces)) for _ in range(4)]
        else:
            links = max(self.size - 1, 1) * self.count
            self.scratch = [dma((links,)), dma((links,))]
        self.scratch.append(dma((2, self.count)))
        if not small:
            self.scratch.append(pltpu.VMEM((self.count,) + block, array.dtype))

    def bind(self, sources, landed, scratch):
        self.source, self.landed, self.bound = sources[0], landed, scratch
        self.own = lax.axis_index(self.axis)
        self.near = self.own + 1 - 2 * lax.rem(self.own, 2)
        self.far = self.own + 2 - 4 * lax.rem(self.own // 2, 2)

    def view(self, target, which, cut=None):
        cut = pl.ds(0, self.block[0]) if cut is None else cut
        if self.mode == "columns":
            return self.source.at[cut, self.lanes(self.slots[which](), self.width)]
        return self.source.at[target if self.mode == "spread" else 0, cut]

    def landing(self, origin, which, cut=None):
        cut = pl.ds(0, self.block[0]) if cut is None else cut
        if self.slots is None:
            return self.landed.at[origin, cut]
        return self.landed.at[origin, cut, self.lanes(self.slots[which](), self.width)]

    def lanes(self, slot, width):
        return pl.ds(pl.multiple_of(slot * width, width), width)

    def direct(self):
        copies = []
        if self.mode == "mate":
            for site in range(self.count):
                slot = 2 * site + lax.rem(self.own, 2)
                place = self.landed.at[:, :, self.lanes(slot, self.landed.shape[-1] // self.size)]
                copies.append((place, place, self.bound[0].at[site], self.bound[1].at[site], self.near))
        else:
            for which in range(self.count):
                for step in range(1, self.size):
                    target = lax.rem(self.own + step, self.size)
                    link = which * (self.size - 1) + step - 1
                    copies.append(
                        (
                            self.view(target, which),
                            self.landing(self.own, which),
                            self.bound[0].at[link],
                            self.bound[1].at[link],
                            target,
                        )
                    )
        return [
            pltpu.make_async_remote_copy(
                src_ref=source,
                dst_ref=place,
                send_sem=send,
                recv_sem=recv,
                device_id={self.axis: target},
            )
            for source, place, send, recv, target in copies
        ]

    def keep(self, leg, which):
        source, place = self.view(self.own, which), self.landing(self.own, which)
        sems = self.bound[4 if self.relay else 2]
        if not self.small:
            stage = self.bound[-1].at[which]
            source, place = (stage, place) if leg else (source, stage)
        return pltpu.make_async_copy(source, place, sems.at[leg, which])

    def rows(self, piece, half=None):
        length = self.block[0] // RELAY_PIECES
        start = (piece % RELAY_PIECES) * length
        if half is None:
            return pl.ds(start, length)
        return pl.ds(start + half * (length // 2), length // 2)

    def first_hop(self, way, piece):
        return pltpu.make_async_remote_copy(
            src_ref=self.view(0, piece // RELAY_PIECES, self.rows(piece)),
            dst_ref=self.landing(self.own, piece // RELAY_PIECES, self.rows(piece)),
            send_sem=self.bound[0].at[way, piece],
            recv_sem=self.bound[1].at[way, piece],
            device_id={"task": self.far if way else self.near},
        )

    def second_hop(self, way, piece):
        place = self.landing(
            self.far if way else self.near, piece // RELAY_PIECES, self.rows(piece, way)
        )
        return pltpu.make_async_remote_copy(
            src_ref=place,
            dst_ref=place,
            send_sem=self.bound[2].at[way, piece],
            recv_sem=self.bound[3].at[way, piece],
            device_id={"task": self.near if way else self.far},
        )

    def start(self):
        for piece in range(self.pieces):
            for way in (0, 1):
                self.first_hop(way, piece).start()
        if not self.relay:
            for copy in self.direct():
                copy.start()
        if self.mode != "mate":
            for which in range(self.count):
                self.keep(0, which).start()

    def advance(self, piece):
        for way in (0, 1):
            self.first_hop(way, piece).wait_recv()
            self.second_hop(way, piece).start()

    def settle(self):
        if self.mode != "mate" and not self.small:
            for which in range(self.count):
                self.keep(0, which).wait()
                self.keep(1, which).start()

    def finish(self):
        if self.mode != "mate":
            for which in range(self.count):
                self.keep(0 if self.small else 1, which).wait()
        for piece in range(self.pieces):
            for way in (0, 1):
                self.first_hop(way, piece).wait_send()
                self.second_hop(way, piece).wait()
        if not self.relay:
            for copy in self.direct():
                copy.wait()


class Riders:
    def __init__(self, riders, main):
        self.riders = riders
        self.todo = [(rider, piece) for rider in riders for piece in range(rider.pieces)]
        self.inputs = [array for rider in riders for array in rider.inputs]
        self.scratch = [item for rider in riders for item in rider.scratch]
        self.shapes = [rider.shape for rider in riders]
        self.in_specs, self.out_specs, self.aliases = [], [], {}
        for i, rider in enumerate(riders):
            space = pl.BlockSpec(memory_space=pltpu.VMEM if rider.small else pltpu.HBM)
            self.in_specs += [space] * len(rider.inputs)
            self.out_specs.append(space)
            if rider.carry is not None:
                self.aliases[main + len(self.in_specs) - 1] = 1 + i
        self.done = 0

    def bind(self, inputs, outputs, scratch):
        inputs, scratch = list(inputs), list(scratch)
        for rider, landed in zip(self.riders, outputs):
            rider.bind(inputs[: len(rider.inputs)], landed, scratch[: len(rider.scratch)])
            inputs = inputs[len(rider.inputs) :]
            scratch = scratch[len(rider.scratch) :]
        self.done = 0

    def start(self):
        for rider in self.riders:
            rider.start()

    def advance(self, numerator, denominator):
        goal = min(len(self.todo), -(-len(self.todo) * numerator // denominator))
        while self.done < goal:
            rider, piece = self.todo[self.done]
            rider.advance(piece)
            self.done += 1

    def settle(self):
        for rider in self.riders:
            rider.settle()

    def finish(self):
        self.advance(1, 1)
        for rider in self.riders:
            rider.finish()


def rider_greeting(riders):
    tp_wide = any(r.axis == "tp" and r.mode != "mate" for r in riders.riders)
    return tp_wide, any(r.axis == "task" for r in riders.riders)


def line_gather_kernel(size, form, pieces, riders, *refs):
    given, count = len(riders.inputs), len(riders.riders)
    source, landed = refs[0], refs[1 + given]
    sems = refs[2 + given + count :]
    up_send, up_recv, down_send, down_recv, mate_send, mate_recv, own_sem, stage = sems[:8]
    riders.bind(refs[1 : 1 + given], refs[2 + given : 2 + given + count], sems[8:])
    own = lax.axis_index("tp")
    core, site, sites = lax.rem(own, 2), own // 2, size // 2
    mate = own + 1 - 2 * core
    greet(own, size, *rider_greeting(riders))

    def hop(step, piece, ahead, origin):
        slot = 2 * origin + core
        place = window(landed, form, size, slot, piece, pieces)
        start = window(source, form, 1, 0, piece, pieces) if step == 0 else place
        return pltpu.make_async_remote_copy(
            src_ref=start,
            dst_ref=place,
            send_sem=(up_send if ahead else down_send).at[step, piece],
            recv_sem=(up_recv if ahead else down_recv).at[step, piece],
            device_id={"tp": own + 2 if ahead else own - 2},
        )

    def pass_on(origin, piece, first):
        place = window(landed, form, size, 2 * origin + core, piece, pieces)
        return pltpu.make_async_remote_copy(
            src_ref=window(source, form, 1, 0, piece, pieces) if first else place,
            dst_ref=place,
            send_sem=mate_send.at[origin, piece],
            recv_sem=mate_recv.at[origin, piece],
            device_id={"tp": mate},
        )

    for piece in range(pieces):

        @pl.when(site < sites - 1)
        def _():
            hop(0, piece, True, site).start()

        @pl.when(site > 0)
        def _():
            hop(0, piece, False, site).start()

    riders.start()

    def keep(leg, piece):
        mine = window(source, form, 1, 0, piece, pieces)
        place = window(landed, form, size, own, piece, pieces)
        held = window(stage, form, 1, 0, piece, pieces)
        return pltpu.make_async_copy(
            held if leg else mine, place if leg else held, own_sem.at[leg, piece]
        )

    for piece in range(pieces):
        pass_on(site, piece, True).start()
        keep(0, piece).start()
    for piece in range(pieces):
        keep(0, piece).wait()
        keep(1, piece).start()
    riders.settle()
    for step in range(1, sites):
        for piece in range(pieces):

            @pl.when(site >= step)
            def _():
                hop(step - 1, piece, True, site - step).wait_recv()

                @pl.when(site < sites - 1)
                def _():
                    hop(step, piece, True, site - step).start()

                pass_on(site - step, piece, False).start()

            @pl.when(site + step < sites)
            def _():
                hop(step - 1, piece, False, site + step).wait_recv()

                @pl.when(site > 0)
                def _():
                    hop(step, piece, False, site + step).start()

                pass_on(site + step, piece, False).start()

        riders.advance(step, sites - 1)

    riders.advance(1, 1)
    for piece in range(pieces):
        keep(1, piece).wait()
    for step in range(sites - 1):
        for piece in range(pieces):

            @pl.when((site >= step) & (site < sites - 1))
            def _():
                hop(step, piece, True, site - step).wait_send()

            @pl.when((site + step < sites) & (site > 0))
            def _():
                hop(step, piece, False, site + step).wait_send()

    for origin in range(sites):
        for piece in range(pieces):
            pass_on(origin, piece, False).wait()

    riders.finish()


def line_gather(block, form, identity, riders=()):
    size = lax.axis_size("tp")
    shape = list(block.shape)
    if form == "cross":
        shape = shape[:1] + [size] + shape[1:]
    else:
        shape[1 if form == "lanes" else 0] *= size
    pieces = 2 if block.shape[-2] % 32 == 0 else 1
    sites = size // 2
    dma = pltpu.SemaphoreType.DMA
    anywhere = pl.BlockSpec(memory_space=pltpu.HBM)
    riders = Riders(riders, 1)
    return pl.pallas_call(
        functools.partial(line_gather_kernel, size, form, pieces, riders),
        out_shape=[jax.ShapeDtypeStruct(tuple(shape), block.dtype)] + riders.shapes,
        in_specs=[anywhere] + riders.in_specs,
        out_specs=[anywhere] + riders.out_specs,
        scratch_shapes=[dma((max(sites - 1, 1), pieces)) for _ in range(4)]
        + [dma((sites, pieces)), dma((sites, pieces)), dma((2, pieces))]
        + [pltpu.VMEM(block.shape, block.dtype)]
        + riders.scratch,
        input_output_aliases=riders.aliases,
        compiler_params=pltpu.CompilerParams(
            collective_id=identity, has_side_effects=True, vmem_limit_bytes=52 * 1024 * 1024
        ),
        cost_estimate=pl.CostEstimate(
            flops=10_000_000_000, bytes_accessed=2 * size * block.size, transcendentals=0
        ),
        name="line_gather",
    )(block, *riders.inputs)


def line_scatter_kernel(size, pieces, riders, *refs):
    given, count = len(riders.inputs), len(riders.riders)
    terms, total = refs[0], refs[1 + given]
    riding, refs = refs[: 2 + given + count], refs[2 + given + count :]
    riders.bind(riding[1 : 1 + given], riding[2 + given :], refs[11:])
    refs = refs[:11]
    mate_in, up_in, down_in, up_out, down_out = refs[:5]
    mate_send, mate_recv, up_send, up_recv, down_send, down_recv = refs[5:]
    own = lax.axis_index("tp")
    core, site, sites = lax.rem(own, 2), own // 2, size // 2
    mate = own + 1 - 2 * core
    rows = terms.shape[1] // pieces
    greet(own, size, *rider_greeting(riders))

    def cut(piece):
        return pl.ds(piece * rows, rows)

    def to_mate(site_of, piece):
        return pltpu.make_async_remote_copy(
            src_ref=terms.at[2 * site_of + 1 - core, cut(piece)],
            dst_ref=mate_in.at[site_of, cut(piece)],
            send_sem=mate_send.at[site_of, piece],
            recv_sem=mate_recv.at[site_of, piece],
            device_id={"tp": mate},
        )

    def hop(site_of, piece, ahead):
        return pltpu.make_async_remote_copy(
            src_ref=(up_out if ahead else down_out).at[site_of, cut(piece)],
            dst_ref=(up_in if ahead else down_in).at[site_of, cut(piece)],
            send_sem=(up_send if ahead else down_send).at[site_of, piece],
            recv_sem=(up_recv if ahead else down_recv).at[site_of, piece],
            device_id={"tp": own + 2 if ahead else own - 2},
        )

    def pair_sum(site_of, piece):
        return terms[2 * site_of + core, cut(piece)].astype(jnp.float32) + mate_in[
            site_of, cut(piece)
        ].astype(jnp.float32)

    order = []
    for far in range((sites + 1) // 2):
        order += [sites - 1 - far] + ([far] if far != sites - 1 - far else [])
    for site_of in order:
        for piece in range(pieces):
            to_mate(site_of, piece).start()
    riders.start()
    for far in range(sites - 1):
        for piece in range(pieces):
            for ahead, site_of in ((True, sites - 1 - far), (False, far)):
                arriving = (site > 0) if ahead else (site < sites - 1)
                outbox = up_out if ahead else down_out
                inbox = up_in if ahead else down_in

                @pl.when((site_of > site) if ahead else (site_of < site))
                def _():
                    to_mate(site_of, piece).wait_recv()

                    @pl.when(arriving)
                    def _():
                        hop(site_of, piece, ahead).wait_recv()
                        outbox[site_of, cut(piece)] = (
                            pair_sum(site_of, piece) + inbox[site_of, cut(piece)].astype(jnp.float32)
                        ).astype(outbox.dtype)

                    @pl.when(jnp.logical_not(arriving))
                    def _():
                        outbox[site_of, cut(piece)] = pair_sum(site_of, piece).astype(outbox.dtype)

                    hop(site_of, piece, ahead).start()

        if far == 0:
            riders.settle()
        riders.advance(far, sites)

    if sites == 1:
        riders.settle()
    riders.advance(1, 1)
    for piece in range(pieces):
        to_mate(site, piece).wait_recv()
        total[cut(piece)] = pair_sum(site, piece)

        @pl.when(site > 0)
        def _():
            hop(site, piece, True).wait_recv()
            total[cut(piece)] += up_in[site, cut(piece)].astype(jnp.float32)

        @pl.when(site < sites - 1)
        def _():
            hop(site, piece, False).wait_recv()
            total[cut(piece)] += down_in[site, cut(piece)].astype(jnp.float32)

    for site_of in range(sites):
        for piece in range(pieces):
            to_mate(site_of, piece).wait_send()

            @pl.when(site_of > site)
            def _():
                hop(site_of, piece, True).wait_send()

            @pl.when(site_of < site)
            def _():
                hop(site_of, piece, False).wait_send()

    riders.finish()


def line_scatter(terms, identity, riders=()):
    size = lax.axis_size("tp")
    sites = size // 2
    rows, width = terms.shape[1:]
    pieces = 2 if rows % 32 == 0 else 1
    dma = pltpu.SemaphoreType.DMA
    box = pltpu.VMEM((sites, rows, width), terms.dtype)
    vmem = pl.BlockSpec(memory_space=pltpu.VMEM)
    riders = Riders(riders, 1)
    return pl.pallas_call(
        functools.partial(line_scatter_kernel, size, pieces, riders),
        out_shape=[jax.ShapeDtypeStruct((rows, width), jnp.float32)] + riders.shapes,
        in_specs=[vmem] + riders.in_specs,
        out_specs=[vmem] + riders.out_specs,
        scratch_shapes=[box] * 5 + [dma((sites, pieces))] * 6 + riders.scratch,
        input_output_aliases=riders.aliases,
        compiler_params=pltpu.CompilerParams(
            collective_id=identity, has_side_effects=True, vmem_limit_bytes=52 * 1024 * 1024
        ),
        cost_estimate=pl.CostEstimate(
            flops=10_000_000_000, bytes_accessed=4 * terms.size, transcendentals=0
        ),
        name="line_scatter",
    )(terms, *riders.inputs)


def exchange_kernel(axis, size, spread, source, landed, send_sems, recv_sems):
    own = lax.axis_index(axis)
    entry = pltpu.get_barrier_semaphore()
    for step in range(1, size):
        pl.semaphore_signal(entry, inc=1, device_id={axis: lax.rem(own + step, size)})
    pl.semaphore_wait(entry, size - 1)
    copies = []
    for step in range(1, size):
        target = lax.rem(own + step, size)
        copy = pltpu.make_async_remote_copy(
            src_ref=source.at[target if spread else 0],
            dst_ref=landed.at[own],
            send_sem=send_sems.at[step - 1],
            recv_sem=recv_sems.at[step - 1],
            device_id={axis: target},
        )
        copy.start()
        copies.append(copy)
    landed[own] = source[own if spread else 0]
    for copy in copies:
        copy.wait()


def exchange(blocks, axis, spread, identity):
    size = lax.axis_size(axis)
    return pl.pallas_call(
        functools.partial(exchange_kernel, axis, size, spread),
        out_shape=jax.ShapeDtypeStruct((size,) + blocks.shape[1:], blocks.dtype),
        in_specs=[pl.BlockSpec(memory_space=pltpu.VMEM)],
        out_specs=pl.BlockSpec(memory_space=pltpu.VMEM),
        scratch_shapes=[
            pltpu.SemaphoreType.DMA((size - 1,)),
            pltpu.SemaphoreType.DMA((size - 1,)),
        ],
        compiler_params=pltpu.CompilerParams(
            collective_id=identity, has_side_effects=True, vmem_limit_bytes=8 * 1024 * 1024
        ),
        cost_estimate=pl.CostEstimate(
            flops=400_000_000, bytes_accessed=2 * blocks.size, transcendentals=0
        ),
    )(blocks)


def task_gather(value):
    tasks, own = lax.axis_size("task"), lax.axis_index("task")
    found = [(own, value)]
    for step in range(1, tasks):
        if tasks & (tasks - 1):
            pairs, origin = [(i, (i + step) % tasks) for i in range(tasks)], (own - step) % tasks
        else:
            pairs, origin = [(i, i ^ step) for i in range(tasks)], own ^ step
        found.append((origin, lax.ppermute(value, "task", pairs)))
    return found


def on_device(
    observations,
    gain,
    w_in,
    w_mix,
    w_out,
    w_head,
    head_bias,
    pop_mean,
    pop_scale,
    task_indices,
    actions,
    rewards,
    episode_ends,
    behaviour_log_prob,
):
    env_count, frames, part_width = observations.shape
    groups = lax.axis_size("tp")
    full_width = part_width * groups
    row_count = env_count * frames
    local_rows = row_count // groups
    own_tokens = observations.reshape(row_count, part_width)
    discount_factors = DISCOUNT * (1.0 - episode_ends.astype(jnp.float32))
    counts, totals, squares = popart_partials(task_indices, rewards, discount_factors)
    count_tasks = counts.shape[0]
    sums = jnp.stack([counts, totals, squares])
    sums = jnp.pad(sums, ((0, 5), (0, -count_tasks % LANES)))
    sites = groups // 2

    def slot_away(away):
        own_now = lax.axis_index("tp")
        return 2 * lax.rem(own_now // 2 + away, sites) + lax.rem(own_now, 2)

    def token_riders(first, last, held):
        slots = tuple(functools.partial(slot_away, away) for away in range(first, min(last, sites)))
        return (Rider(tokens, "task", "columns", slots, part_width, held),) if slots else ()

    tokens, gain_all, tokens_all = line_gather(
        own_tokens,
        "lanes",
        0,
        (
            Rider(gain.reshape(1, -1, LANES), "tp", small=True),
            Rider(own_tokens[None], "task", slots=(functools.partial(slot_away, 0),)),
        ),
    )
    row_offset = lax.axis_index("tp") * local_rows
    token_rows = lax.dynamic_slice_in_dim(tokens, row_offset, local_rows, 0)
    pre_in = jnp.dot(tokens, w_in, preferred_element_type=jnp.float32)
    hidden_in = jax.nn.silu(pre_in).astype(jnp.bfloat16)
    mix_terms = jnp.dot(hidden_in, w_mix, preferred_element_type=jnp.float32).astype(jnp.bfloat16)
    mix_sum, all_sums, hidden_all, *held = line_scatter(
        mix_terms.reshape(groups, local_rows, full_width),
        1,
        (Rider(sums[None], "task", small=True), Rider(hidden_in[None], "task"))
        + token_riders(1, 2, tokens_all),
    )
    tokens_all = held[0] if held else tokens_all
    gain_all = gain_all.reshape(full_width)
    counts, totals, squares = jnp.sum(all_sums, axis=0)[:3, :count_tasks]
    updated_return_mean, updated_return_scale = popart_update(
        counts, totals, squares, pop_mean, pop_scale
    )
    new_head, new_bias = rescale_head(
        w_head, head_bias, pop_mean, pop_scale, updated_return_mean, updated_return_scale
    )
    loss_weighting = float(env_count * lax.axis_size("task")) ** (-0.5)
    heads = new_head.shape[1]
    wide_head = jnp.pad(new_head, ((0, 0), (0, -heads % LANES)))
    residual = token_rows.astype(jnp.float32) + mix_sum
    inverse = lax.rsqrt(jnp.mean(residual * residual, axis=1, keepdims=True) + NORM_EPS)
    normed = (residual * inverse * gain_all[None, :]).astype(jnp.bfloat16)
    normed_all, *held = line_gather(normed, "rows", 2, token_riders(2, sites, tokens_all))
    tokens_all = held[0] if held else tokens_all
    pre_out = jnp.dot(normed_all, w_out, preferred_element_type=jnp.float32)
    hidden_out = jax.nn.silu(pre_out).astype(jnp.bfloat16)
    head_terms = jnp.dot(hidden_out, wide_head, preferred_element_type=jnp.float32)
    head_blocks = head_terms.astype(jnp.bfloat16).reshape(groups, local_rows, -1)
    head_sum = jnp.sum(exchange(head_blocks, "tp", True, 3).astype(jnp.float32), axis=0)
    head_value_estimates = head_sum[:, :heads] + new_bias[None, :]
    own_envs = env_count // groups
    head_value_estimates = head_value_estimates.reshape(own_envs, frames, heads)

    def own(values):
        return lax.dynamic_slice_in_dim(values, lax.axis_index("tp") * own_envs, own_envs, 0)

    def group_loss(network_outputs):
        return importance_trace_loss(
            network_outputs,
            own(task_indices),
            own(actions),
            own(rewards),
            own(discount_factors),
            own(behaviour_log_prob),
            updated_return_mean,
            updated_return_scale,
            loss_weighting,
        )

    loss_value, pullback = jax.vjp(group_loss, head_value_estimates)
    (d_heads,) = pullback(jnp.ones((), jnp.float32))
    d_own = d_heads.reshape(local_rows, heads).astype(jnp.bfloat16)
    d_own = jnp.pad(d_own, ((0, 0), (0, -heads % LANES)))
    d_rounded = exchange(d_own[None], "tp", False, 4).reshape(row_count, -1)
    d_hidden_out = jnp.dot(d_rounded, wide_head.T, preferred_element_type=jnp.float32)
    d_pre_out = (d_hidden_out * silu_slope(pre_out)).astype(jnp.bfloat16)
    d_terms = jnp.dot(d_pre_out, w_out.T, preferred_element_type=jnp.float32)
    d_terms = d_terms.astype(jnp.bfloat16)
    grad_out = jnp.dot(normed_all.T, d_pre_out, preferred_element_type=jnp.float32)
    grad_head = jnp.dot(hidden_out.T, d_rounded, preferred_element_type=jnp.float32)
    grad_bias = jnp.sum(d_rounded.astype(jnp.float32), axis=0)
    tasks = lax.axis_size("task")
    out_quarter, quarter = full_width // tasks, full_width // tasks
    d_normed, grad_out, grad_head = line_scatter(
        d_terms.reshape(groups, local_rows, full_width),
        5,
        (
            Rider(
                grad_out.astype(jnp.bfloat16).reshape(tasks, out_quarter, part_width),
                "task",
                "spread",
            ),
            Rider(grad_head.astype(jnp.bfloat16)[None], "task", small=True),
        ),
    )
    grad_out = jnp.sum(grad_out.astype(jnp.float32), axis=0).astype(jnp.bfloat16)
    grad_head = jnp.sum(grad_head.astype(jnp.float32), axis=0)[:, :heads]
    scaled = d_normed * gain_all[None, :]
    inner_sum = jnp.sum(scaled * residual, axis=1, keepdims=True)
    d_residual = (inverse * scaled - residual * inverse**3 * inner_sum / full_width).astype(
        jnp.bfloat16
    )
    gain_terms = jnp.sum(d_normed * residual * inverse, axis=0).reshape(groups, -1, LANES)
    half = quarter // 2
    d_quarters = d_residual.reshape(local_rows, tasks, quarter).transpose(1, 0, 2)
    arrived, gain_blocks, grad_out, d_quarters = line_gather(
        d_residual,
        "rows",
        6,
        (
            Rider(gain_terms, "tp", "spread", small=True),
            Rider(grad_out[None], "task"),
            Rider(d_quarters, "task", "spread"),
        ),
    )
    d_hidden = jnp.dot(arrived, w_mix.T, preferred_element_type=jnp.float32)
    d_pre_in = (d_hidden * silu_slope(pre_in)).astype(jnp.bfloat16)
    gain_block = jnp.sum(gain_blocks, axis=0)
    bias_block = grad_bias.reshape(-1, LANES)
    small = jnp.concatenate([gain_block, bias_block], axis=0)
    small = jnp.pad(small, ((0, -small.shape[0] % 8), (0, 0)))
    own_task = lax.axis_index("task")

    def foreign(blocks):
        others = [lax.rem(own_task + step, tasks) for step in range(1, tasks)]
        return jnp.stack([lax.dynamic_index_in_dim(blocks, i, 0, keepdims=False) for i in others])

    d_foreign, hidden_foreign = foreign(d_quarters), foreign(hidden_all)
    hidden_foreign = hidden_foreign.reshape(-1, part_width)

    def mix_half(d_cross, which):
        own_columns = lax.dynamic_slice_in_dim(arrived, own_task * quarter + which * half, half, 1)
        others = jnp.dot(
            hidden_foreign.T, d_cross.reshape(-1, half), preferred_element_type=jnp.float32
        )
        mine = jnp.dot(hidden_in.T, own_columns, preferred_element_type=jnp.float32)
        return (others + mine).astype(jnp.bfloat16)

    d_cross, d_pre_in, small, tokens_all = line_gather(
        d_foreign[..., :half],
        "cross",
        7,
        (
            Rider(d_pre_in[None], "task"),
            Rider(small[None], "task", small=True),
            Rider(None, "tp", "mate", carry=tokens_all),
        ),
    )
    mix_first = mix_half(d_cross, 0)
    d_cross, mix_first = line_gather(
        d_foreign[..., half:], "cross", 8, (Rider(mix_first[None], "task"),)
    )
    mix_second, d_pre_in, grad_out, small, mix_first = lax.optimization_barrier(
        (mix_half(d_cross, 1), d_pre_in, grad_out, small, mix_first)
    )
    found = task_gather(mix_second)
    small = jnp.sum(small, axis=0)
    gain_rows = gain_block.shape[0]
    grad_gain = small[:gain_rows].reshape(part_width)
    grad_bias = small[gain_rows : gain_rows + bias_block.shape[0]].reshape(-1)[:heads]
    every_row = tasks * row_count
    grad_in = jnp.dot(
        tokens_all.reshape(every_row, full_width).T,
        d_pre_in.reshape(every_row, part_width),
        preferred_element_type=jnp.float32,
    )
    grad_out = grad_out.reshape(full_width, part_width).astype(jnp.float32)
    grad_mix = jnp.zeros((part_width, full_width), jnp.float32)
    for task in range(tasks):
        grad_mix = lax.dynamic_update_slice_in_dim(
            grad_mix, mix_first[task].astype(jnp.float32), task * quarter, 1
        )
    arrivals, grad_in, grad_out, grad_mix = lax.optimization_barrier(
        ([value for _, value in found], grad_in, grad_out, grad_mix)
    )
    for (task, _), value in zip(found, arrivals):
        grad_mix = lax.dynamic_update_slice_in_dim(
            grad_mix, value.astype(jnp.float32), task * quarter + half, 1
        )
    return (
        grad_in,
        grad_mix,
        grad_out,
        grad_gain,
        grad_head,
        grad_bias,
        new_head,
        new_bias,
        updated_return_mean,
        updated_return_scale,
    )


def solution(mesh):
    in_specs = (
        P("task", None, "tp"),
        P("tp"),
        P(None, "tp"),
        P("tp", None),
        P(None, "tp"),
        P("tp", None),
        P(),
        P(),
        P(),
        P("task"),
        P("task", None),
        P("task", None),
        P("task", None),
        P("task", None),
    )
    out_specs = (
        P(None, "tp"),
        P("tp", None),
        P(None, "tp"),
        P("tp"),
        P("tp", None),
        P(),
        P("tp", None),
        P(),
        P(),
        P(),
    )
    return jax.shard_map(
        on_device, mesh=mesh, in_specs=in_specs, out_specs=out_specs, check_vma=False
    )
```

```python
import functools

import jax
import jax.numpy as jnp
from jax import lax
from jax.experimental import pallas as pl
from jax.experimental.pallas import tpu as pltpu
from jax.sharding import PartitionSpec as P

LANES = 128

ACTIONS = 18
TASKS = 57


DISCOUNT = 0.99
BASELINE_COST = 0.5
ENTROPY_COST = 0.01
POPART_PRIOR = 64.0
NORM_EPS = 1e-06


def silu_slope(before):
    sigmoid = jax.nn.sigmoid(before)
    return sigmoid * (1.0 + before * (1.0 - sigmoid))


def discounted_sums(values, factors):
    step = 1
    while step < values.shape[1]:
        pad = ((0, 0), (0, step))
        values = values + factors * jnp.pad(values[:, step:], pad)
        factors = factors * jnp.pad(factors[:, step:], pad)
        step *= 2
    return values


def task_onehot(task_indices):
    return (task_indices[:, None] == jnp.arange(TASKS, dtype=jnp.int32)[None, :]).astype(
        jnp.float32
    )


def popart_partials(task_indices, rewards, discount_factors):
    returns = discounted_sums(rewards, discount_factors)
    task_table = task_onehot(task_indices)
    counts = jnp.sum(task_table, axis=0) * rewards.shape[1]
    totals = jnp.dot(task_table.T, jnp.sum(returns, axis=1), precision=lax.Precision.HIGHEST)
    squares = jnp.dot(
        task_table.T, jnp.sum(returns * returns, axis=1), precision=lax.Precision.HIGHEST
    )
    return (counts, totals, squares)


def popart_update(counts, totals, squares, pop_mean, pop_scale):
    mixing = counts / (counts + POPART_PRIOR)
    safe_counts = jnp.maximum(counts, 1.0)
    batch_mean = totals / safe_counts
    batch_square = squares / safe_counts
    updated_return_mean = (1.0 - mixing) * pop_mean + mixing * batch_mean
    mean_gap = batch_mean - pop_mean
    variance = (
        (1.0 - mixing) * pop_scale * pop_scale
        + mixing * (batch_square - batch_mean * batch_mean)
        + mixing * (1.0 - mixing) * mean_gap * mean_gap
    )
    return (updated_return_mean, jnp.sqrt(variance))


def rescale_head(w_head, head_bias, pop_mean, pop_scale, updated_return_mean, updated_return_scale):
    scale_ratio = pop_scale / updated_return_scale
    column_scale = jnp.concatenate([jnp.ones((ACTIONS,), jnp.float32), scale_ratio])
    new_head = (w_head.astype(jnp.float32) * column_scale[None, :]).astype(jnp.bfloat16)
    value_bias = (
        pop_scale * head_bias[ACTIONS:] + pop_mean - updated_return_mean
    ) / updated_return_scale
    new_bias = jnp.concatenate([head_bias[:ACTIONS], value_bias])
    return (new_head, new_bias)


def importance_trace_loss(
    head_value_estimates,
    task_indices,
    actions,
    rewards,
    discount_factors,
    behaviour_log_prob,
    updated_return_mean,
    updated_return_scale,
    loss_weighting,
):
    task_table = task_onehot(task_indices)
    env_mean = jnp.dot(task_table, updated_return_mean, precision=lax.Precision.HIGHEST)[:, None]
    env_scale = jnp.dot(task_table, updated_return_scale, precision=lax.Precision.HIGHEST)[:, None]
    logits = head_value_estimates[:, :-1, :ACTIONS]
    norm_values = jnp.sum(head_value_estimates[:, :, ACTIONS:] * task_table[:, None, :], axis=2)
    values = lax.stop_gradient(norm_values * env_scale + env_mean)
    log_total = jnp.log(jnp.sum(jnp.exp(logits), axis=2))
    chosen = actions[:, :, None] == jnp.arange(ACTIONS, dtype=jnp.int32)[None, None, :]
    log_policy = jnp.sum(jnp.where(chosen, logits, 0.0), axis=2) - log_total
    clipped = jnp.minimum(jnp.exp(lax.stop_gradient(log_policy) - behaviour_log_prob), 1.0)
    deltas = clipped * (rewards + discount_factors * values[:, 1:] - values[:, :-1])
    targets = values[:, :-1] + discounted_sums(deltas, discount_factors * clipped)
    following = jnp.concatenate([targets[:, 1:], values[:, -1:]], axis=1)
    advantage = lax.stop_gradient(
        clipped
        * ((rewards + discount_factors * following - env_mean) / env_scale - norm_values[:, :-1])
    )
    normed_targets = lax.stop_gradient((targets - env_mean) / env_scale)
    policy = jnp.exp(logits - log_total[:, :, None])
    entropy = -jnp.sum(policy * (logits - log_total[:, :, None]), axis=2)
    per_frame = (
        -advantage * log_policy
        + 0.5 * BASELINE_COST * (normed_targets - norm_values[:, :-1]) ** 2
        - ENTROPY_COST * entropy
    )
    return loss_weighting * jnp.sum(per_frame)


def window(ref, form, slots, slot, piece, pieces):
    if form == "lanes":
        rows, width = ref.shape[0] // pieces, ref.shape[1] // slots
        start = slot * width if slots == 1 else pl.multiple_of(slot * width, width)
        return ref.at[pl.ds(piece * rows, rows), pl.ds(start, width)]
    if form == "rows":
        height = ref.shape[0] // slots
        rows = height // pieces
        return ref.at[pl.ds(pl.multiple_of(slot * height + piece * rows, rows), rows)]
    rows = ref.shape[-2] // pieces
    cut = pl.ds(piece * rows, rows)
    return ref.at[:, cut] if slots == 1 else ref.at[:, slot, cut]


def greet(own, size, everyone, task_too):
    entry = pltpu.get_barrier_semaphore()
    expected = 0
    if everyone:
        for step in range(1, size):
            pl.semaphore_signal(entry, inc=1, device_id={"tp": lax.rem(own + step, size)})
        expected = size - 1
    else:
        below, above = own >= 2, own < size - 2
        pl.semaphore_signal(entry, inc=1, device_id={"tp": own + 1 - 2 * lax.rem(own, 2)})

        @pl.when(below)
        def _():
            pl.semaphore_signal(entry, inc=1, device_id={"tp": own - 2})

        @pl.when(above)
        def _():
            pl.semaphore_signal(entry, inc=1, device_id={"tp": own + 2})

        expected = 1 + below.astype(jnp.int32) + above.astype(jnp.int32)
    if task_too:
        tasks = lax.axis_size("task")
        task = lax.axis_index("task")
        for step in range(1, tasks):
            pl.semaphore_signal(entry, inc=1, device_id={"task": lax.rem(task + step, tasks)})
        expected = expected + tasks - 1
    pl.semaphore_wait(entry, expected)


RELAY_PIECES = 2


class Rider:
    def __init__(self, array, axis, mode="same", slots=None, width=None, carry=None, small=False):
        self.axis, self.mode, self.small = axis, mode, small
        self.size = lax.axis_size(axis)
        self.carry = carry
        self.inputs = [] if array is None else [array]
        self.inputs += [] if carry is None else [carry]
        self.slots = slots
        self.width = width
        dma = pltpu.SemaphoreType.DMA
        if mode == "mate":
            self.shape = jax.ShapeDtypeStruct(carry.shape, carry.dtype)
            self.relay, self.pieces, self.count = False, 0, self.size // 2
            self.scratch = [dma((self.count,)), dma((self.count,))]
            return
        block = (array.shape[0], width) if mode == "columns" else array.shape[1:]
        self.block = block
        shape = (self.size,) + block
        if slots is not None:
            self.width = block[-1]
            shape = shape[:-1] + (lax.axis_size("tp") * self.width,)
        self.shape = jax.ShapeDtypeStruct(shape, array.dtype)
        self.relay = (
            not small
            and axis == "task"
            and self.size == 4
            and mode in ("same", "columns")
            and block[0] % (32 * RELAY_PIECES) == 0
        )
        self.count = 1 if slots is None else len(slots)
        self.pieces = RELAY_PIECES * self.count if self.relay else 0
        if self.relay:
            self.scratch = [dma((2, self.pieces)) for _ in range(4)]
        else:
            links = max(self.size - 1, 1) * self.count
            self.scratch = [dma((links,)), dma((links,))]
        self.scratch.append(dma((2, self.count)))
        if not small:
            self.scratch.append(pltpu.VMEM((self.count,) + block, array.dtype))

    def bind(self, sources, landed, scratch):
        self.source, self.landed, self.bound = sources[0], landed, scratch
        self.own = lax.axis_index(self.axis)
        self.near = self.own + 1 - 2 * lax.rem(self.own, 2)
        self.far = self.own + 2 - 4 * lax.rem(self.own // 2, 2)

    def view(self, target, which, cut=None):
        cut = pl.ds(0, self.block[0]) if cut is None else cut
        if self.mode == "columns":
            return self.source.at[cut, self.lanes(self.slots[which](), self.width)]
        return self.source.at[target if self.mode == "spread" else 0, cut]

    def landing(self, origin, which, cut=None):
        cut = pl.ds(0, self.block[0]) if cut is None else cut
        if self.slots is None:
            return self.landed.at[origin, cut]
        return self.landed.at[origin, cut, self.lanes(self.slots[which](), self.width)]

    def lanes(self, slot, width):
        return pl.ds(pl.multiple_of(slot * width, width), width)

    def direct(self):
        copies = []
        if self.mode == "mate":
            for site in range(self.count):
                slot = 2 * site + lax.rem(self.own, 2)
                place = self.landed.at[:, :, self.lanes(slot, self.landed.shape[-1] // self.size)]
                copies.append((place, place, self.bound[0].at[site], self.bound[1].at[site], self.near))
        else:
            for which in range(self.count):
                for step in range(1, self.size):
                    target = lax.rem(self.own + step, self.size)
                    link = which * (self.size - 1) + step - 1
                    copies.append(
                        (
                            self.view(target, which),
                            self.landing(self.own, which),
                            self.bound[0].at[link],
                            self.bound[1].at[link],
                            target,
                        )
                    )
        return [
            pltpu.make_async_remote_copy(
                src_ref=source,
                dst_ref=place,
                send_sem=send,
                recv_sem=recv,
                device_id={self.axis: target},
            )
            for source, place, send, recv, target in copies
        ]

    def keep(self, leg, which):
        source, place = self.view(self.own, which), self.landing(self.own, which)
        sems = self.bound[4 if self.relay else 2]
        if not self.small:
            stage = self.bound[-1].at[which]
            source, place = (stage, place) if leg else (source, stage)
        return pltpu.make_async_copy(source, place, sems.at[leg, which])

    def rows(self, piece, half=None):
        length = self.block[0] // RELAY_PIECES
        start = (piece % RELAY_PIECES) * length
        if half is None:
            return pl.ds(start, length)
        return pl.ds(start + half * (length // 2), length // 2)

    def first_hop(self, way, piece):
        return pltpu.make_async_remote_copy(
            src_ref=self.view(0, piece // RELAY_PIECES, self.rows(piece)),
            dst_ref=self.landing(self.own, piece // RELAY_PIECES, self.rows(piece)),
            send_sem=self.bound[0].at[way, piece],
            recv_sem=self.bound[1].at[way, piece],
            device_id={"task": self.far if way else self.near},
        )

    def second_hop(self, way, piece):
        place = self.landing(
            self.far if way else self.near, piece // RELAY_PIECES, self.rows(piece, way)
        )
        return pltpu.make_async_remote_copy(
            src_ref=place,
            dst_ref=place,
            send_sem=self.bound[2].at[way, piece],
            recv_sem=self.bound[3].at[way, piece],
            device_id={"task": self.near if way else self.far},
        )

    def start(self):
        for piece in range(self.pieces):
            for way in (0, 1):
                self.first_hop(way, piece).start()
        if not self.relay:
            for copy in self.direct():
                copy.start()
        if self.mode != "mate":
            for which in range(self.count):
                self.keep(0, which).start()

    def advance(self, piece):
        for way in (0, 1):
            self.first_hop(way, piece).wait_recv()
            self.second_hop(way, piece).start()

    def settle(self):
        if self.mode != "mate" and not self.small:
            for which in range(self.count):
                self.keep(0, which).wait()
                self.keep(1, which).start()

    def finish(self):
        if self.mode != "mate":
            for which in range(self.count):
                self.keep(0 if self.small else 1, which).wait()
        for piece in range(self.pieces):
            for way in (0, 1):
                self.first_hop(way, piece).wait_send()
                self.second_hop(way, piece).wait()
        if not self.relay:
            for copy in self.direct():
                copy.wait()


class Reducer:
    def __init__(self, array):
        tasks, rows, width = array.shape
        self.axis, self.mode, self.small, self.carry = "task", "reduce", True, None
        self.inputs, self.pieces, self.half = [array], 1, rows // 2
        self.shape = jax.ShapeDtypeStruct((1, rows, width), array.dtype)
        dma, piece = pltpu.SemaphoreType.DMA, (rows // 2, width)
        self.scratch = [dma((2, 2))] * 2 + [dma((2,))] * 2
        self.scratch += [pltpu.VMEM((2, 2) + piece, array.dtype)]
        self.scratch += [pltpu.VMEM((2,) + piece, array.dtype)] * 2

    def bind(self, sources, landed, scratch):
        self.source, self.landed = sources[0], landed
        self.send, self.recv, self.send_last, self.recv_last = scratch[:4]
        self.inbox, self.outbox, self.last = scratch[4:]
        self.own = lax.axis_index("task")
        near = self.own + 1 - 2 * lax.rem(self.own, 2)
        far = self.own + 2 - 4 * lax.rem(self.own // 2, 2)
        self.around = ((near, far), (far, near))
        self.across = near + far - self.own

    def cut(self, way):
        return pl.ds(way * self.half, self.half)

    def first(self, way, which):
        partner = self.around[way][0]
        return pltpu.make_async_remote_copy(
            src_ref=self.source.at[self.across if which else partner, self.cut(way)],
            dst_ref=self.inbox.at[way, which],
            send_sem=self.send.at[way, which],
            recv_sem=self.recv.at[way, which],
            device_id={"task": partner},
        )

    def second(self, way):
        return pltpu.make_async_remote_copy(
            src_ref=self.outbox.at[way],
            dst_ref=self.last.at[way],
            send_sem=self.send_last.at[way],
            recv_sem=self.recv_last.at[way],
            device_id={"task": self.around[way][1]},
        )

    def start(self):
        for which in (1, 0):
            for way in (0, 1):
                self.first(way, which).start()

    def sum_of(self, block, way, which):
        mine = self.source[block, self.cut(way)].astype(jnp.float32)
        return mine + self.inbox[way, which].astype(jnp.float32)

    def advance(self, piece):
        for way in (0, 1):
            self.first(way, 1).wait_recv()
            self.outbox[way] = self.sum_of(self.around[way][1], way, 1).astype(self.outbox.dtype)
            self.second(way).start()

    def settle(self):
        pass

    def finish(self):
        for way in (0, 1):
            self.first(way, 0).wait_recv()
            held = self.sum_of(self.own, way, 0)
            self.second(way).wait_recv()
            self.landed[0, self.cut(way)] = (held + self.last[way].astype(jnp.float32)).astype(
                self.landed.dtype
            )
        for way in (0, 1):
            self.second(way).wait_send()
            for which in (0, 1):
                self.first(way, which).wait_send()


class Riders:
    def __init__(self, riders, main):
        self.riders = riders
        self.todo = [(rider, piece) for rider in riders for piece in range(rider.pieces)]
        self.inputs = [array for rider in riders for array in rider.inputs]
        self.scratch = [item for rider in riders for item in rider.scratch]
        self.shapes = [rider.shape for rider in riders]
        self.in_specs, self.out_specs, self.aliases = [], [], {}
        for i, rider in enumerate(riders):
            space = pl.BlockSpec(memory_space=pltpu.VMEM if rider.small else pltpu.HBM)
            self.in_specs += [space] * len(rider.inputs)
            self.out_specs.append(space)
            if rider.carry is not None:
                self.aliases[main + len(self.in_specs) - 1] = 1 + i
        self.done = 0

    def bind(self, inputs, outputs, scratch):
        inputs, scratch = list(inputs), list(scratch)
        for rider, landed in zip(self.riders, outputs):
            rider.bind(inputs[: len(rider.inputs)], landed, scratch[: len(rider.scratch)])
            inputs = inputs[len(rider.inputs) :]
            scratch = scratch[len(rider.scratch) :]
        self.done = 0

    def start(self):
        for rider in self.riders:
            rider.start()

    def advance(self, numerator, denominator):
        goal = min(len(self.todo), len(self.todo) * numerator // denominator)
        while self.done < goal:
            rider, piece = self.todo[self.done]
            rider.advance(piece)
            self.done += 1

    def settle(self):
        for rider in self.riders:
            rider.settle()

    def finish(self):
        self.advance(1, 1)
        for rider in self.riders:
            rider.finish()


def rider_greeting(riders):
    tp_wide = any(r.axis == "tp" and r.mode != "mate" for r in riders.riders)
    return tp_wide, any(r.axis == "task" for r in riders.riders)


def line_gather_kernel(size, form, pieces, riders, *refs):
    given, count = len(riders.inputs), len(riders.riders)
    source, landed = refs[0], refs[1 + given]
    sems = refs[2 + given + count :]
    up_send, up_recv, down_send, down_recv, mate_send, mate_recv, own_sem, stage = sems[:8]
    riders.bind(refs[1 : 1 + given], refs[2 + given : 2 + given + count], sems[8:])
    own = lax.axis_index("tp")
    core, site, sites = lax.rem(own, 2), own // 2, size // 2
    mate = own + 1 - 2 * core
    greet(own, size, *rider_greeting(riders))

    def hop(step, piece, ahead, origin):
        slot = 2 * origin + core
        place = window(landed, form, size, slot, piece, pieces)
        start = window(source, form, 1, 0, piece, pieces) if step == 0 else place
        return pltpu.make_async_remote_copy(
            src_ref=start,
            dst_ref=place,
            send_sem=(up_send if ahead else down_send).at[step, piece],
            recv_sem=(up_recv if ahead else down_recv).at[step, piece],
            device_id={"tp": own + 2 if ahead else own - 2},
        )

    def pass_on(origin, piece, first):
        place = window(landed, form, size, 2 * origin + core, piece, pieces)
        return pltpu.make_async_remote_copy(
            src_ref=window(source, form, 1, 0, piece, pieces) if first else place,
            dst_ref=place,
            send_sem=mate_send.at[origin, piece],
            recv_sem=mate_recv.at[origin, piece],
            device_id={"tp": mate},
        )

    for piece in range(pieces):

        @pl.when(site < sites - 1)
        def _():
            hop(0, piece, True, site).start()

        @pl.when(site > 0)
        def _():
            hop(0, piece, False, site).start()

    riders.start()

    def keep(leg, piece):
        mine = window(source, form, 1, 0, piece, pieces)
        place = window(landed, form, size, own, piece, pieces)
        held = window(stage, form, 1, 0, piece, pieces)
        return pltpu.make_async_copy(
            held if leg else mine, place if leg else held, own_sem.at[leg, piece]
        )

    for piece in range(pieces):
        pass_on(site, piece, True).start()
        keep(0, piece).start()
    for piece in range(pieces):
        keep(0, piece).wait()
        keep(1, piece).start()
    riders.settle()
    for step in range(1, sites):
        for piece in range(pieces):

            @pl.when(site >= step)
            def _():
                hop(step - 1, piece, True, site - step).wait_recv()

                @pl.when(site < sites - 1)
                def _():
                    hop(step, piece, True, site - step).start()

                pass_on(site - step, piece, False).start()

            @pl.when(site + step < sites)
            def _():
                hop(step - 1, piece, False, site + step).wait_recv()

                @pl.when(site > 0)
                def _():
                    hop(step, piece, False, site + step).start()

                pass_on(site + step, piece, False).start()

        riders.advance(step * len(riders.todo) + sites - 2, (sites - 1) * max(len(riders.todo), 1))

    riders.advance(1, 1)
    for piece in range(pieces):
        keep(1, piece).wait()
    for step in range(sites - 1):
        for piece in range(pieces):

            @pl.when((site >= step) & (site < sites - 1))
            def _():
                hop(step, piece, True, site - step).wait_send()

            @pl.when((site + step < sites) & (site > 0))
            def _():
                hop(step, piece, False, site + step).wait_send()

    for origin in range(sites):
        for piece in range(pieces):
            pass_on(origin, piece, False).wait()

    riders.finish()


def line_gather(block, form, identity, riders=()):
    size = lax.axis_size("tp")
    shape = list(block.shape)
    if form == "cross":
        shape = shape[:1] + [size] + shape[1:]
    else:
        shape[1 if form == "lanes" else 0] *= size
    pieces = 2 if block.shape[-2] % 32 == 0 else 1
    sites = size // 2
    dma = pltpu.SemaphoreType.DMA
    anywhere = pl.BlockSpec(memory_space=pltpu.HBM)
    riders = Riders(riders, 1)
    return pl.pallas_call(
        functools.partial(line_gather_kernel, size, form, pieces, riders),
        out_shape=[jax.ShapeDtypeStruct(tuple(shape), block.dtype)] + riders.shapes,
        in_specs=[anywhere] + riders.in_specs,
        out_specs=[anywhere] + riders.out_specs,
        scratch_shapes=[dma((max(sites - 1, 1), pieces)) for _ in range(4)]
        + [dma((sites, pieces)), dma((sites, pieces)), dma((2, pieces))]
        + [pltpu.VMEM(block.shape, block.dtype)]
        + riders.scratch,
        input_output_aliases=riders.aliases,
        compiler_params=pltpu.CompilerParams(
            collective_id=identity, has_side_effects=True, vmem_limit_bytes=52 * 1024 * 1024
        ),
        cost_estimate=pl.CostEstimate(
            flops=10_000_000_000, bytes_accessed=2 * size * block.size, transcendentals=0
        ),
        name="line_gather",
    )(block, *riders.inputs)


def line_scatter_kernel(size, pieces, riders, *refs):
    given, count = len(riders.inputs), len(riders.riders)
    terms, total = refs[0], refs[1 + given]
    riding, refs = refs[: 2 + given + count], refs[2 + given + count :]
    riders.bind(riding[1 : 1 + given], riding[2 + given :], refs[11:])
    refs = refs[:11]
    mate_in, up_in, down_in, up_out, down_out = refs[:5]
    mate_send, mate_recv, up_send, up_recv, down_send, down_recv = refs[5:]
    own = lax.axis_index("tp")
    core, site, sites = lax.rem(own, 2), own // 2, size // 2
    mate = own + 1 - 2 * core
    rows = terms.shape[1] // pieces
    greet(own, size, *rider_greeting(riders))

    def cut(piece):
        return pl.ds(piece * rows, rows)

    def to_mate(site_of, piece):
        return pltpu.make_async_remote_copy(
            src_ref=terms.at[2 * site_of + 1 - core, cut(piece)],
            dst_ref=mate_in.at[site_of, cut(piece)],
            send_sem=mate_send.at[site_of, piece],
            recv_sem=mate_recv.at[site_of, piece],
            device_id={"tp": mate},
        )

    def hop(site_of, piece, ahead):
        return pltpu.make_async_remote_copy(
            src_ref=(up_out if ahead else down_out).at[site_of, cut(piece)],
            dst_ref=(up_in if ahead else down_in).at[site_of, cut(piece)],
            send_sem=(up_send if ahead else down_send).at[site_of, piece],
            recv_sem=(up_recv if ahead else down_recv).at[site_of, piece],
            device_id={"tp": own + 2 if ahead else own - 2},
        )

    def pair_sum(site_of, piece):
        return terms[2 * site_of + core, cut(piece)].astype(jnp.float32) + mate_in[
            site_of, cut(piece)
        ].astype(jnp.float32)

    order = []
    for far in range((sites + 1) // 2):
        order += [sites - 1 - far] + ([far] if far != sites - 1 - far else [])
    for site_of in order:
        for piece in range(pieces):
            to_mate(site_of, piece).start()
    riders.start()
    for far in range(sites - 1):
        for piece in range(pieces):
            for ahead, site_of in ((True, sites - 1 - far), (False, far)):
                arriving = (site > 0) if ahead else (site < sites - 1)
                outbox = up_out if ahead else down_out
                inbox = up_in if ahead else down_in

                @pl.when((site_of > site) if ahead else (site_of < site))
                def _():
                    to_mate(site_of, piece).wait_recv()

                    @pl.when(arriving)
                    def _():
                        hop(site_of, piece, ahead).wait_recv()
                        outbox[site_of, cut(piece)] = (
                            pair_sum(site_of, piece) + inbox[site_of, cut(piece)].astype(jnp.float32)
                        ).astype(outbox.dtype)

                    @pl.when(jnp.logical_not(arriving))
                    def _():
                        outbox[site_of, cut(piece)] = pair_sum(site_of, piece).astype(outbox.dtype)

                    hop(site_of, piece, ahead).start()

        if far == 0:
            riders.settle()
        riders.advance(far, sites)

    if sites == 1:
        riders.settle()
    riders.advance(1, 1)
    for piece in range(pieces):
        to_mate(site, piece).wait_recv()
        total[cut(piece)] = pair_sum(site, piece)

        @pl.when(site > 0)
        def _():
            hop(site, piece, True).wait_recv()
            total[cut(piece)] += up_in[site, cut(piece)].astype(jnp.float32)

        @pl.when(site < sites - 1)
        def _():
            hop(site, piece, False).wait_recv()
            total[cut(piece)] += down_in[site, cut(piece)].astype(jnp.float32)

    for site_of in range(sites):
        for piece in range(pieces):
            to_mate(site_of, piece).wait_send()

            @pl.when(site_of > site)
            def _():
                hop(site_of, piece, True).wait_send()

            @pl.when(site_of < site)
            def _():
                hop(site_of, piece, False).wait_send()

    riders.finish()


def line_scatter(terms, identity, riders=()):
    size = lax.axis_size("tp")
    sites = size // 2
    rows, width = terms.shape[1:]
    pieces = 2 if rows % 32 == 0 else 1
    dma = pltpu.SemaphoreType.DMA
    box = pltpu.VMEM((sites, rows, width), terms.dtype)
    vmem = pl.BlockSpec(memory_space=pltpu.VMEM)
    riders = Riders(riders, 1)
    return pl.pallas_call(
        functools.partial(line_scatter_kernel, size, pieces, riders),
        out_shape=[jax.ShapeDtypeStruct((rows, width), jnp.float32)] + riders.shapes,
        in_specs=[vmem] + riders.in_specs,
        out_specs=[vmem] + riders.out_specs,
        scratch_shapes=[box] * 5 + [dma((sites, pieces))] * 6 + riders.scratch,
        input_output_aliases=riders.aliases,
        compiler_params=pltpu.CompilerParams(
            collective_id=identity, has_side_effects=True, vmem_limit_bytes=52 * 1024 * 1024
        ),
        cost_estimate=pl.CostEstimate(
            flops=10_000_000_000, bytes_accessed=4 * terms.size, transcendentals=0
        ),
        name="line_scatter",
    )(terms, *riders.inputs)


def exchange_kernel(axis, size, spread, source, landed, send_sems, recv_sems):
    own = lax.axis_index(axis)
    entry = pltpu.get_barrier_semaphore()
    for step in range(1, size):
        pl.semaphore_signal(entry, inc=1, device_id={axis: lax.rem(own + step, size)})
    pl.semaphore_wait(entry, size - 1)
    copies = []
    for step in range(1, size):
        target = lax.rem(own + step, size)
        copy = pltpu.make_async_remote_copy(
            src_ref=source.at[target if spread else 0],
            dst_ref=landed.at[own],
            send_sem=send_sems.at[step - 1],
            recv_sem=recv_sems.at[step - 1],
            device_id={axis: target},
        )
        copy.start()
        copies.append(copy)
    landed[own] = source[own if spread else 0]
    for copy in copies:
        copy.wait()


def exchange(blocks, axis, spread, identity):
    size = lax.axis_size(axis)
    return pl.pallas_call(
        functools.partial(exchange_kernel, axis, size, spread),
        out_shape=jax.ShapeDtypeStruct((size,) + blocks.shape[1:], blocks.dtype),
        in_specs=[pl.BlockSpec(memory_space=pltpu.VMEM)],
        out_specs=pl.BlockSpec(memory_space=pltpu.VMEM),
        scratch_shapes=[
            pltpu.SemaphoreType.DMA((size - 1,)),
            pltpu.SemaphoreType.DMA((size - 1,)),
        ],
        compiler_params=pltpu.CompilerParams(
            collective_id=identity, has_side_effects=True, vmem_limit_bytes=8 * 1024 * 1024
        ),
        cost_estimate=pl.CostEstimate(
            flops=400_000_000, bytes_accessed=2 * blocks.size, transcendentals=0
        ),
    )(blocks)


def lay_out_kernel(origins, first, *refs):
    seconds, whole = refs[:-1], refs[-1]
    half = first.shape[-1]
    whole[:, :half] = first[0].astype(jnp.float32)
    for step, second in enumerate(seconds):

        @pl.when(pl.program_id(0) == step)
        def _():
            whole[:, half:] = second[...].astype(jnp.float32)


def lay_out(first, seconds, origins):
    tasks, rows, half = first.shape
    return pl.pallas_call(
        lay_out_kernel,
        grid_spec=pltpu.PrefetchScalarGridSpec(
            num_scalar_prefetch=1,
            grid=(tasks,),
            in_specs=[pl.BlockSpec((1, rows, half), lambda i, order: (order[i], 0, 0))]
            + [pl.BlockSpec((rows, half), lambda i, order: (0, 0))] * tasks,
            out_specs=pl.BlockSpec((rows, 2 * half), lambda i, order: (0, order[i])),
        ),
        out_shape=jax.ShapeDtypeStruct((rows, 2 * half * tasks), jnp.float32),
        compiler_params=pltpu.CompilerParams(vmem_limit_bytes=40 * 1024 * 1024),
        cost_estimate=pl.CostEstimate(
            flops=100_000_000, bytes_accessed=12 * tasks * rows * half, transcendentals=0
        ),
        name="lay_out",
    )(origins.astype(jnp.int32), first, *seconds)


def task_gather(value):
    tasks, own = lax.axis_size("task"), lax.axis_index("task")
    found = [(own, value)]
    for step in range(1, tasks):
        if tasks & (tasks - 1):
            pairs, origin = [(i, (i + step) % tasks) for i in range(tasks)], (own - step) % tasks
        else:
            pairs, origin = [(i, i ^ step) for i in range(tasks)], own ^ step
        found.append((origin, lax.ppermute(value, "task", pairs)))
    return found


def on_device(
    observations,
    gain,
    w_in,
    w_mix,
    w_out,
    w_head,
    head_bias,
    pop_mean,
    pop_scale,
    task_indices,
    actions,
    rewards,
    episode_ends,
    behaviour_log_prob,
):
    env_count, frames, part_width = observations.shape
    groups = lax.axis_size("tp")
    full_width = part_width * groups
    row_count = env_count * frames
    local_rows = row_count // groups
    own_tokens = observations.reshape(row_count, part_width)
    discount_factors = DISCOUNT * (1.0 - episode_ends.astype(jnp.float32))
    counts, totals, squares = popart_partials(task_indices, rewards, discount_factors)
    count_tasks = counts.shape[0]
    sums = jnp.stack([counts, totals, squares])
    sums = jnp.pad(sums, ((0, 5), (0, -count_tasks % LANES)))
    sites = groups // 2

    def slot_away(away):
        own_now = lax.axis_index("tp")
        return 2 * lax.rem(own_now // 2 + away, sites) + lax.rem(own_now, 2)

    def token_riders(first, last, held):
        slots = tuple(functools.partial(slot_away, away) for away in range(first, min(last, sites)))
        return (Rider(tokens, "task", "columns", slots, part_width, held),) if slots else ()

    tokens, gain_all, tokens_all = line_gather(
        own_tokens,
        "lanes",
        0,
        (
            Rider(gain.reshape(1, -1, LANES), "tp", small=True),
            Rider(own_tokens[None], "task", slots=(functools.partial(slot_away, 0),)),
        ),
    )
    row_offset = lax.axis_index("tp") * local_rows
    token_rows = lax.dynamic_slice_in_dim(tokens, row_offset, local_rows, 0)
    pre_in = jnp.dot(tokens, w_in, preferred_element_type=jnp.float32)
    hidden_in = jax.nn.silu(pre_in).astype(jnp.bfloat16)
    mix_terms = jnp.dot(hidden_in, w_mix, preferred_element_type=jnp.float32).astype(jnp.bfloat16)
    mix_sum, all_sums, hidden_all, *held = line_scatter(
        mix_terms.reshape(groups, local_rows, full_width),
        1,
        (Rider(sums[None], "task", small=True), Rider(hidden_in[None], "task"))
        + token_riders(1, 2, tokens_all),
    )
    tokens_all = held[0] if held else tokens_all
    gain_all = gain_all.reshape(full_width)
    counts, totals, squares = jnp.sum(all_sums, axis=0)[:3, :count_tasks]
    updated_return_mean, updated_return_scale = popart_update(
        counts, totals, squares, pop_mean, pop_scale
    )
    new_head, new_bias = rescale_head(
        w_head, head_bias, pop_mean, pop_scale, updated_return_mean, updated_return_scale
    )
    loss_weighting = float(env_count * lax.axis_size("task")) ** (-0.5)
    heads = new_head.shape[1]
    wide_head = jnp.pad(new_head, ((0, 0), (0, -heads % LANES)))
    residual = token_rows.astype(jnp.float32) + mix_sum
    inverse = lax.rsqrt(jnp.mean(residual * residual, axis=1, keepdims=True) + NORM_EPS)
    normed = (residual * inverse * gain_all[None, :]).astype(jnp.bfloat16)
    normed_all, *held = line_gather(normed, "rows", 2, token_riders(2, sites, tokens_all))
    tokens_all = held[0] if held else tokens_all
    pre_out = jnp.dot(normed_all, w_out, preferred_element_type=jnp.float32)
    hidden_out = jax.nn.silu(pre_out).astype(jnp.bfloat16)
    head_terms = jnp.dot(hidden_out, wide_head, preferred_element_type=jnp.float32)
    head_blocks = head_terms.astype(jnp.bfloat16).reshape(groups, local_rows, -1)
    head_sum = jnp.sum(exchange(head_blocks, "tp", True, 3).astype(jnp.float32), axis=0)
    head_value_estimates = head_sum[:, :heads] + new_bias[None, :]
    own_envs = env_count // groups
    head_value_estimates = head_value_estimates.reshape(own_envs, frames, heads)

    def own(values):
        return lax.dynamic_slice_in_dim(values, lax.axis_index("tp") * own_envs, own_envs, 0)

    def group_loss(network_outputs):
        return importance_trace_loss(
            network_outputs,
            own(task_indices),
            own(actions),
            own(rewards),
            own(discount_factors),
            own(behaviour_log_prob),
            updated_return_mean,
            updated_return_scale,
            loss_weighting,
        )

    loss_value, pullback = jax.vjp(group_loss, head_value_estimates)
    (d_heads,) = pullback(jnp.ones((), jnp.float32))
    d_own = d_heads.reshape(local_rows, heads).astype(jnp.bfloat16)
    d_own = jnp.pad(d_own, ((0, 0), (0, -heads % LANES)))
    d_rounded = exchange(d_own[None], "tp", False, 4).reshape(row_count, -1)
    d_hidden_out = jnp.dot(d_rounded, wide_head.T, preferred_element_type=jnp.float32)
    d_pre_out = (d_hidden_out * silu_slope(pre_out)).astype(jnp.bfloat16)
    d_terms = jnp.dot(d_pre_out, w_out.T, preferred_element_type=jnp.float32)
    d_terms = d_terms.astype(jnp.bfloat16)
    grad_out = jnp.dot(normed_all.T, d_pre_out, preferred_element_type=jnp.float32)
    grad_head = jnp.dot(hidden_out.T, d_rounded, preferred_element_type=jnp.float32)
    grad_bias = jnp.sum(d_rounded.astype(jnp.float32), axis=0)
    tasks = lax.axis_size("task")
    out_quarter, quarter = full_width // tasks, full_width // tasks
    grad_out = grad_out.astype(jnp.bfloat16).reshape(tasks, out_quarter, part_width)
    halving = tasks == 4 and out_quarter % 32 == 0
    d_normed, grad_out, grad_head = line_scatter(
        d_terms.reshape(groups, local_rows, full_width),
        5,
        (
            Reducer(grad_out) if halving else Rider(grad_out, "task", "spread"),
            Rider(grad_head.astype(jnp.bfloat16)[None], "task", small=True),
        ),
    )
    if not halving:
        grad_out = jnp.sum(grad_out.astype(jnp.float32), axis=0).astype(jnp.bfloat16)[None]
    grad_head = jnp.sum(grad_head.astype(jnp.float32), axis=0)[:, :heads]
    scaled = d_normed * gain_all[None, :]
    inner_sum = jnp.sum(scaled * residual, axis=1, keepdims=True)
    d_residual = (inverse * scaled - residual * inverse**3 * inner_sum / full_width).astype(
        jnp.bfloat16
    )
    gain_terms = jnp.sum(d_normed * residual * inverse, axis=0).reshape(groups, -1, LANES)
    half = quarter // 2
    d_quarters = d_residual.reshape(local_rows, tasks, quarter).transpose(1, 0, 2)
    arrived, gain_blocks, grad_out, d_quarters = line_gather(
        d_residual,
        "rows",
        6,
        (
            Rider(gain_terms, "tp", "spread", small=True),
            Rider(grad_out, "task"),
            Rider(d_quarters, "task", "spread"),
        ),
    )
    d_hidden = jnp.dot(arrived, w_mix.T, preferred_element_type=jnp.float32)
    d_pre_in = (d_hidden * silu_slope(pre_in)).astype(jnp.bfloat16)
    gain_block = jnp.sum(gain_blocks, axis=0)
    bias_block = grad_bias.reshape(-1, LANES)
    small = jnp.concatenate([gain_block, bias_block], axis=0)
    small = jnp.pad(small, ((0, -small.shape[0] % 8), (0, 0)))
    own_task = lax.axis_index("task")

    def foreign(blocks):
        others = [lax.rem(own_task + step, tasks) for step in range(1, tasks)]
        return jnp.stack([lax.dynamic_index_in_dim(blocks, i, 0, keepdims=False) for i in others])

    d_foreign, hidden_foreign = foreign(d_quarters), foreign(hidden_all)
    hidden_foreign = hidden_foreign.reshape(-1, part_width)

    def mix_half(d_cross, which):
        own_columns = lax.dynamic_slice_in_dim(arrived, own_task * quarter + which * half, half, 1)
        others = jnp.dot(
            hidden_foreign.T, d_cross.reshape(-1, half), preferred_element_type=jnp.float32
        )
        mine = jnp.dot(hidden_in.T, own_columns, preferred_element_type=jnp.float32)
        return (others + mine).astype(jnp.bfloat16)

    d_cross, d_pre_in, small, tokens_all = line_gather(
        d_foreign[..., :half],
        "cross",
        7,
        (
            Rider(d_pre_in[None], "task"),
            Rider(small[None], "task", small=True),
            Rider(None, "tp", "mate", carry=tokens_all),
        ),
    )
    mix_first = mix_half(d_cross, 0)
    d_cross, mix_first = line_gather(
        d_foreign[..., half:], "cross", 8, (Rider(mix_first[None], "task"),)
    )
    mix_second, d_pre_in, grad_out, small, mix_first = lax.optimization_barrier(
        (mix_half(d_cross, 1), d_pre_in, grad_out, small, mix_first)
    )
    found = task_gather(mix_second)
    small = jnp.sum(small, axis=0)
    gain_rows = gain_block.shape[0]
    grad_gain = small[:gain_rows].reshape(part_width)
    grad_bias = small[gain_rows : gain_rows + bias_block.shape[0]].reshape(-1)[:heads]
    every_row = tasks * row_count
    grad_in = jnp.dot(
        tokens_all.reshape(every_row, full_width).T,
        d_pre_in.reshape(every_row, part_width),
        preferred_element_type=jnp.float32,
    )
    grad_out = grad_out.reshape(full_width, part_width).astype(jnp.float32)
    arrivals, mix_first, grad_in, grad_out = lax.optimization_barrier(
        ([value for _, value in found], mix_first, grad_in, grad_out)
    )
    grad_mix = lay_out(mix_first, arrivals, jnp.stack([task for task, _ in found]))
    return (
        grad_in,
        grad_mix,
        grad_out,
        grad_gain,
        grad_head,
        grad_bias,
        new_head,
        new_bias,
        updated_return_mean,
        updated_return_scale,
    )


def solution(mesh):
    in_specs = (
        P("task", None, "tp"),
        P("tp"),
        P(None, "tp"),
        P("tp", None),
        P(None, "tp"),
        P("tp", None),
        P(),
        P(),
        P(),
        P("task"),
        P("task", None),
        P("task", None),
        P("task", None),
        P("task", None),
    )
    out_specs = (
        P(None, "tp"),
        P("tp", None),
        P(None, "tp"),
        P("tp"),
        P("tp", None),
        P(),
        P("tp", None),
        P(),
        P(),
        P(),
    )
    return jax.shard_map(
        on_device, mesh=mesh, in_specs=in_specs, out_specs=out_specs, check_vma=False
    )
```
